32 devices in a mesh: dp: 1 (over z), tp: 4 (over y), cp: 8 (over x, core).
Axes of the slice: x: 4, y: 4, z: 1, core: 2. Of those that a mesh axis runs over, the one named last changes fastest.
The devices are a block of a 4x4x8 slice.
Arguments:
- x: bfloat16 [8192, 5120], P(('dp', 'cp'))
- attn_gain: bfloat16 [5120], replicated
- w_q: bfloat16 [5120, 4096], P(None, 'tp')
- w_k: bfloat16 [5120, 1024], P(None, 'tp')
- w_v: bfloat16 [5120, 1024], P(None, 'tp')
- w_o: bfloat16 [4096, 5120], P('tp')
- mlp_gain: bfloat16 [5120], replicated
- w_gate: bfloat16 [5120, 14336], P(None, 'tp')
- w_up: bfloat16 [5120, 14336], P(None, 'tp')
- w_down: bfloat16 [14336, 5120], P('tp')
Outputs:
- output 1: bfloat16 [8192, 5120], P(('dp', 'cp'))
- output 2: bfloat16 [8192, 8, 128], P(('dp', 'cp'), 'tp')
- output 3: bfloat16 [8192, 8, 128], P(('dp', 'cp'), 'tp')
All inputs are finite; a program needn't handle non-finite values.
Results may differ from the reference program's by a relative error of at most 0.0135963.
Values are sent between devices in bfloat16 or wider.
A program may use at most 768 MiB of HBM per device.

```python
import jax
import jax.numpy as jnp
from jax import lax

SEQ_LEN = 8192
MODEL_DIM = 5120
FF_DIM = 14336
NUM_HEADS = 32
KV_HEADS = 8
HEAD_DIM = 128
ROPE_THETA = 1000000
BLOCK_LEN = 256
NORM_EPS = 1e-5
MASK_VALUE = -1e30


def setup_inputs(seed: int = 0, part: int = 0) -> dict:
    root = jax.random.key(seed)
    key_list = jax.random.split(root, 10)
    seq_key = jax.random.fold_in(key_list[0], part)
    noise_key, dir_key, freq_key, phase_key = jax.random.split(seq_key, 4)
    seq_frac = jnp.arange(SEQ_LEN, dtype=jnp.float32) / SEQ_LEN
    wave_freq = jax.random.uniform(freq_key, (4,), jnp.float32, 0.3, 2.0)
    wave_phase = jax.random.uniform(phase_key, (4,), jnp.float32, 0.0, 6.2831853)
    waves = jnp.cos(6.2831853 * seq_frac[:, None] * wave_freq[None, :] + wave_phase[None, :])
    directions = 0.5 * jax.random.normal(dir_key, (4, MODEL_DIM), jnp.float32)
    noise = jax.random.normal(noise_key, (SEQ_LEN, MODEL_DIM), jnp.float32)
    x = (0.6 * noise + jnp.dot(waves, directions)).astype(jnp.bfloat16)
    q_cols = NUM_HEADS * HEAD_DIM
    kv_cols = KV_HEADS * HEAD_DIM

    def weight(key, rows, cols):
        return (jax.random.normal(key, (rows, cols), jnp.float32) * rows ** -0.5).astype(jnp.bfloat16)

    def gain(key):
        return jax.random.uniform(key, (MODEL_DIM,), jnp.float32, 0.5, 1.5).astype(jnp.bfloat16)

    return {
        'x': x,
        'attn_gain': gain(key_list[1]),
        'w_q': weight(key_list[2], MODEL_DIM, q_cols),
        'w_k': weight(key_list[3], MODEL_DIM, kv_cols),
        'w_v': weight(key_list[4], MODEL_DIM, kv_cols),
        'w_o': weight(key_list[5], q_cols, MODEL_DIM),
        'mlp_gain': gain(key_list[6]),
        'w_gate': weight(key_list[7], MODEL_DIM, FF_DIM),
        'w_up': weight(key_list[8], MODEL_DIM, FF_DIM),
        'w_down': weight(key_list[9], FF_DIM, MODEL_DIM),
    }


def rms_norm(rows, gain):
    wide = rows.astype(jnp.float32)
    inv_rms = lax.rsqrt(jnp.mean(wide * wide, axis=-1, keepdims=True) + NORM_EPS)
    return (wide * inv_rms * gain.astype(jnp.float32)).astype(jnp.bfloat16)


def rope_tables(positions):
    inv_freq = jnp.asarray(ROPE_THETA, jnp.float32) ** (-jnp.arange(0, HEAD_DIM, 2, dtype=jnp.float32) / HEAD_DIM)
    angles = positions.astype(jnp.float32)[:, None] * inv_freq[None, :]
    return jnp.cos(angles), jnp.sin(angles)


def apply_rope(heads, cos_b, sin_b):
    half = HEAD_DIM // 2
    wide = heads.astype(jnp.float32)
    first = wide[..., :half]
    second = wide[..., half:]
    return jnp.concatenate([first * cos_b - second * sin_b, second * cos_b + first * sin_b], axis=-1).astype(jnp.bfloat16)


def causal_attention(queries, keys, values):
    groups = NUM_HEADS // KV_HEADS
    n_blocks = SEQ_LEN // BLOCK_LEN
    q_blocks = queries.reshape(n_blocks, BLOCK_LEN, KV_HEADS, groups, HEAD_DIM)
    k_blocks = keys.reshape(n_blocks, BLOCK_LEN, KV_HEADS, HEAD_DIM)
    v_blocks = values.reshape(n_blocks, BLOCK_LEN, KV_HEADS, HEAD_DIM)
    offsets = jnp.arange(BLOCK_LEN)
    block_ids = jnp.arange(n_blocks)

    def one_query_block(operands):
        q_blk, q_idx = operands
        q_wide = q_blk.astype(jnp.float32)
        q_pos = q_idx * BLOCK_LEN + offsets

        def key_step(carry, inputs):
            run_max, run_sum, weighted = carry
            k_blk, v_blk, k_idx = inputs
            k_pos = k_idx * BLOCK_LEN + offsets
            scores = jnp.einsum('qkgd,skd->kgqs', q_wide, k_blk.astype(jnp.float32)) * (HEAD_DIM ** -0.5)
            scores = jnp.where(k_pos[None, :] <= q_pos[:, None], scores, MASK_VALUE)
            new_max = jnp.maximum(run_max, jnp.max(scores, axis=-1))
            rescale = jnp.exp(run_max - new_max)
            exp_scores = jnp.exp(scores - new_max[..., None])
            new_sum = run_sum * rescale + jnp.sum(exp_scores, axis=-1)
            exp_rounded = exp_scores.astype(jnp.bfloat16).astype(jnp.float32)
            new_weighted = weighted * rescale[..., None] + jnp.einsum('kgqs,skd->kgqd', exp_rounded, v_blk.astype(jnp.float32))
            return (new_max, new_sum, new_weighted), None

        stat_shape = (KV_HEADS, groups, BLOCK_LEN)
        init = (jnp.full(stat_shape, MASK_VALUE, jnp.float32), jnp.zeros(stat_shape, jnp.float32), jnp.zeros(stat_shape + (HEAD_DIM,), jnp.float32))
        final, unused = lax.scan(key_step, init, (k_blocks, v_blocks, block_ids))
        block_out = final[2] / final[1][..., None]
        return jnp.transpose(block_out, (2, 0, 1, 3)).astype(jnp.bfloat16)

    outs = lax.map(one_query_block, (q_blocks, block_ids))
    return outs.reshape(SEQ_LEN, NUM_HEADS * HEAD_DIM)


def reference(x, attn_gain, w_q, w_k, w_v, w_o, mlp_gain, w_gate, w_up, w_down):
    groups = NUM_HEADS // KV_HEADS
    cos_tab, sin_tab = rope_tables(jnp.arange(SEQ_LEN))
    normed = rms_norm(x, attn_gain)
    queries = jnp.dot(normed, w_q, preferred_element_type=jnp.float32).astype(jnp.bfloat16).reshape(SEQ_LEN, NUM_HEADS, HEAD_DIM)
    keys = jnp.dot(normed, w_k, preferred_element_type=jnp.float32).astype(jnp.bfloat16).reshape(SEQ_LEN, KV_HEADS, HEAD_DIM)
    values = jnp.dot(normed, w_v, preferred_element_type=jnp.float32).astype(jnp.bfloat16).reshape(SEQ_LEN, KV_HEADS, HEAD_DIM)
    queries = apply_rope(queries, cos_tab[:, None, :], sin_tab[:, None, :])
    keys = apply_rope(keys, cos_tab[:, None, :], sin_tab[:, None, :])
    attn_rows = causal_attention(queries.reshape(SEQ_LEN, KV_HEADS, groups, HEAD_DIM), keys, values)
    attn_proj = jnp.dot(attn_rows, w_o, preferred_element_type=jnp.float32)
    hidden = (x.astype(jnp.float32) + attn_proj).astype(jnp.bfloat16)
    normed_mlp = rms_norm(hidden, mlp_gain)
    gate_proj = jnp.dot(normed_mlp, w_gate, preferred_element_type=jnp.float32)
    up_proj = jnp.dot(normed_mlp, w_up, preferred_element_type=jnp.float32)
    activated = (jax.nn.silu(gate_proj) * up_proj).astype(jnp.bfloat16)
    down_proj = jnp.dot(activated, w_down, preferred_element_type=jnp.float32)
    x_out = (hidden.astype(jnp.float32) + down_proj).astype(jnp.bfloat16)
    return (x_out, keys, values)
```

```python
import functools
import math
import jax
import jax.numpy as jnp
from jax import lax
from jax.experimental import pallas as pl
from jax.experimental.pallas import tpu as pltpu
from jax.sharding import PartitionSpec as P

HEAD_DIM = 128
ROPE_THETA = 1000000.0
NORM_EPS = 1e-5
MASK_VALUE = -1e30
VMEM_LIMIT = 66000000
HALVES = 2
GROUPS_OUT = 4
FF_TILE = 256
OUT_TILE = 256
PROJ_TILE = 256
Q_CHUNKS = 4
KEY_TILE = 512
OUT_COLS = 1024
NORM_ROWS = 64


def attn_kernel(n_tp, n_cp, x_hbm, gain_ref, mlp_gain_ref, cos_ref, sin_ref, wq_hbm, wk_hbm, wv_hbm, wo_hbm,
                k_out, v_out, h_out, n_out,
                nbuf, wt, kbuf, vbuf, qt, part, relay, fin, hrow, nrow, orow, acc, m_st, l_st, knat, vnat,
                xsem, wsem, wosem, hsem, osem, kvo_sem, kx_send, kx_recv, sb_send, sb_recv, rs_send, rs_recv):
    tok, D = nbuf.shape
    kv_n, groups = kbuf.shape[2], qt.shape[3] // (tok // Q_CHUNKS)
    QC = tok // Q_CHUNKS
    QL = qt.shape[3]
    R = QC // n_tp
    H = R // 2
    lo, hi = pl.ds(0, H), pl.ds(H, H)
    me = lax.axis_index('tp')
    right = lax.rem(me + 1, n_tp)
    left = lax.rem(me + n_tp - 1, n_tp)
    far = lax.rem(me + 2, n_tp)
    cp = lax.axis_index('cp')
    core = lax.rem(cp, 2)
    chip = cp // 2
    sib = cp + 1 - 2 * core
    x_right = lax.rem(cp + 2, n_cp)
    x_left = lax.rem(cp + n_cp - 2, n_cp)
    cexp = (HEAD_DIM ** -0.5) * math.log2(math.e)
    f32, bf16 = jnp.float32, jnp.bfloat16

    def remote(src, dst, ssem, rsem, to):
        return pltpu.make_async_remote_copy(src_ref=src, dst_ref=dst, send_sem=ssem, recv_sem=rsem,
                                            device_id=to, device_id_type=pl.DeviceIdType.MESH)

    def kx(k):
        buf, src, dst, to = ((kbuf, 0, 1, x_right), (vbuf, 0, 1, x_right), (vbuf, 0, 2, x_left), (kbuf, 0, 2, x_left),
                             (kbuf, 1, 3, x_right), (vbuf, 2, 3, x_left))[k]
        return remote(buf.at[src, 0], buf.at[dst, 0], kx_send.at[k], kx_recv.at[k], {'cp': to})

    def sb(rel, b):
        buf = (kbuf, vbuf)[b]
        return remote(buf.at[rel, 0], buf.at[rel, 1], sb_send.at[rel, b], sb_recv.at[rel, b], {'cp': sib})

    def rs(i, k):
        p = lax.rem(i, 2)
        src, dst, to = ((part.at[p, far, lo], relay.at[i, 0], right),
                        (part.at[p, far, hi], relay.at[i, 1], left),
                        (part.at[p, right, hi], fin.at[i, 0, hi], right),
                        (part.at[p, left, lo], fin.at[i, 1, lo], left),
                        (part.at[p, right, lo], fin.at[i, 0, lo], right),
                        (part.at[p, left, hi], fin.at[i, 1, hi], left))[k]
        return remote(src, dst, rs_send.at[i, k], rs_recv.at[i, k], {'tp': to})

    def x_load(c):
        rows = pl.ds(c * QC, QC)
        return pltpu.make_async_copy(x_hbm.at[rows], nbuf.at[rows], xsem.at[c])

    def w_load(ref, t, slot):
        return pltpu.make_async_copy(ref.at[:, pl.ds(pl.multiple_of(t * PROJ_TILE, PROJ_TILE), PROJ_TILE)], wt.at[slot], wsem.at[slot])

    def h_load(i):
        return pltpu.make_async_copy(x_hbm.at[pl.ds(pl.multiple_of(i * QC + me * R, R), R)], hrow.at[i], hsem.at[i])

    def o_store(i):
        rows = pl.ds(i * R, R)
        return (pltpu.make_async_copy(hrow.at[i], h_out.at[rows], osem.at[0, i]),
                pltpu.make_async_copy(nrow.at[i], n_out.at[rows], osem.at[1, i]))

    wo_load = pltpu.make_async_copy(wo_hbm, nbuf, wosem)

    for c in range(Q_CHUNKS):
        x_load(c).start()
    w_load(wk_hbm, 0, 0).start()
    w_load(wv_hbm, 0, 1).start()
    for i in range(Q_CHUNKS):
        h_load(i).start()
    barrier = pltpu.get_barrier_semaphore()
    for to in ({'tp': left}, {'tp': right}, {'cp': x_left}, {'cp': x_right}, {'cp': sib}):
        pl.semaphore_signal(barrier, inc=1, device_id=to, device_id_type=pl.DeviceIdType.MESH)
    pl.semaphore_wait(barrier, 5)

    def normalize(wide, gain):
        inv = lax.rsqrt(jnp.mean(wide * wide, axis=-1, keepdims=True) + NORM_EPS)
        return (wide * inv * gain).astype(bf16)

    gain = gain_ref[...].astype(f32)
    for c in range(Q_CHUNKS):
        x_load(c).wait()

        def norm_step(b, carry):
            rows = pl.ds(pl.multiple_of(c * QC + b * NORM_ROWS, NORM_ROWS), NORM_ROWS)
            nbuf[rows, :] = normalize(nbuf[rows, :].astype(f32), gain)
            return carry
        lax.fori_loop(0, QC // NORM_ROWS, norm_step, 0)

    def rope(u):
        wide = u.astype(bf16).astype(f32)
        return (wide * cos_ref[...] + pltpu.roll(wide, HEAD_DIM // 2, 1) * sin_ref[...]).astype(bf16)

    def project(slot):
        return jnp.dot(nbuf[...], wt[slot], preferred_element_type=f32)

    w_load(wk_hbm, 0, 0).wait()
    res = project(0)
    for j in range(kv_n):
        head = rope(res[:, j * HEAD_DIM:(j + 1) * HEAD_DIM])
        kbuf[0, 0, j] = head
        knat[:, j * HEAD_DIM:(j + 1) * HEAD_DIM] = head
    w_load(wq_hbm, 0, 0).start()
    w_load(wv_hbm, 0, 1).wait()
    kx(0).start()
    kx(3).start()
    sb(0, 0).start()
    res = project(1).astype(bf16)
    vnat[...] = res
    for j in range(kv_n):
        vbuf[0, 0, j] = res[:, j * HEAD_DIM:(j + 1) * HEAD_DIM].T
    w_load(wq_hbm, 1, 1).start()
    pltpu.make_async_copy(knat, k_out, kvo_sem.at[0]).start()
    kx(1).start()
    kx(2).start()
    sb(0, 1).start()
    pltpu.make_async_copy(vnat, v_out, kvo_sem.at[1]).start()

    n_q = wq_hbm.shape[1] // PROJ_TILE
    heads_tile = PROJ_TILE // HEAD_DIM
    tiles_kv = n_q // kv_n

    def q_step(t, carry):
        slot = lax.rem(t, 2)
        w_load(wq_hbm, t, slot).wait()
        res = project(slot)
        kv, base = t // tiles_kv, lax.rem(t, tiles_kv) * heads_tile
        for j in range(heads_tile):
            head = rope(res[:, j * HEAD_DIM:(j + 1) * HEAD_DIM])
            lanes = pl.ds(pl.multiple_of((base + j) * QC, QC), QC)
            for i in range(Q_CHUNKS):
                qt[i, kv, :, lanes] = head[i * QC:(i + 1) * QC].T

        @pl.when(t + 2 < n_q)
        def _():
            w_load(wq_hbm, t + 2, slot).start()

        @pl.when(t == n_q - 1)
        def _():
            kx(0).wait_recv()
            kx(4).start()
            sb(1, 0).start()
            kx(2).wait_recv()
            kx(5).start()
            sb(2, 1).start()
        return carry
    lax.fori_loop(0, n_q, q_step, 0)
    wo_load.start()

    def attend(i, kv, k_tile, v_tile, masked):
        s = jnp.dot(k_tile, qt[i, kv], preferred_element_type=f32)
        if masked:
            key = lax.broadcasted_iota(jnp.int32, s.shape, 0)
            row = lax.broadcasted_iota(jnp.int32, s.shape, 1) & (QC - 1)
            s = jnp.where(key <= row, s, MASK_VALUE)
        m_old = m_st[kv]
        m_new = jnp.maximum(m_old, jnp.max(s, axis=0, keepdims=True))
        alpha = jnp.exp2((m_old - m_new) * cexp)
        p = jnp.exp2((s - m_new) * cexp)
        m_st[kv] = m_new
        l_st[kv] = l_st[kv] * alpha + jnp.sum(p, axis=0, keepdims=True)
        acc[kv] = acc[kv] * alpha + jnp.dot(v_tile, p.astype(bf16), preferred_element_type=f32)

    def m0(i):
        for k in range(4):
            rs(i, k).start()

    def m1(i):
        p = lax.rem(i, 2)
        for j, owner, rows in ((0, right, lo), (1, left, hi)):
            rs(i, j).wait_recv()
            part[p, owner, rows, :] = (part[p, owner, rows, :].astype(f32) + relay[i, j].astype(f32)).astype(bf16)
        rs(i, 4).start()
        rs(i, 5).start()

    mlp_gain = mlp_gain_ref[...].astype(f32)

    def m2(i):
        p = lax.rem(i, 2)
        for k in range(2, 6):
            rs(i, k).wait_recv()
        for k in range(6):
            rs(i, k).wait_send()
        total = part[p, me].astype(f32) + fin[i, 0].astype(f32) + fin[i, 1].astype(f32)
        hid = (hrow[i].astype(f32) + total).astype(bf16)
        hrow[i] = hid
        nrow[i] = normalize(hid.astype(f32), mlp_gain)
        for c in o_store(i):
            c.start()

    def slot_wait(slot):
        rel, is_sib = slot // 2, slot % 2
        if is_sib:
            for b in range(2):
                sb(rel, b).wait_recv()
        elif rel == 1:
            kx(1).wait_recv()
            sb(1, 1).start()
        elif rel == 2:
            kx(3).wait_recv()
            sb(2, 0).start()
        elif rel == 3:
            kx(4).wait_recv()
            kx(5).wait_recv()
            sb(3, 0).start()
            sb(3, 1).start()

    def chunk(i, carry):
        for kv in range(kv_n):
            m_st[kv] = jnp.full((1, QL), MASK_VALUE, f32)
            l_st[kv] = jnp.zeros((1, QL), f32)
            acc[kv] = jnp.zeros((HEAD_DIM, QL), f32)
        for kv in range(kv_n):
            rows = pl.ds(pl.multiple_of(i * QC, QC), QC)
            attend(i, kv, kbuf[0, 0, kv, rows, :], vbuf[0, 0, kv, :, rows], True)

        def diag_step(j, c2):
            rows = pl.ds(pl.multiple_of(j * QC, QC), QC)
            for kv in range(kv_n):
                attend(i, kv, kbuf[0, 0, kv, rows, :], vbuf[0, 0, kv, :, rows], False)
            return c2
        lax.fori_loop(0, i, diag_step, 0)

        def slot_step(slot, c2):
            rel, is_sib = slot // 2, lax.rem(slot, 2)
            for known in range(1, n_cp):
                @pl.when((i == 0) & (slot == known))
                def _():
                    slot_wait(known)
            from_chip = lax.rem(chip + jnp.where(rel == 1, 3, jnp.where(rel == 2, 1, jnp.where(rel == 3, 2, 0))), n_cp // 2)
            from_core = jnp.where(is_sib == 1, 1 - core, core)

            @pl.when(from_chip * 2 + from_core < cp)
            def _():
                def tile_step(j, c3):
                    rows = pl.ds(pl.multiple_of(j * KEY_TILE, KEY_TILE), KEY_TILE)
                    for kv in range(kv_n):
                        attend(i, kv, kbuf[rel, is_sib, kv, rows, :], vbuf[rel, is_sib, kv, :, rows], False)
                    return c3
                lax.fori_loop(0, tok // KEY_TILE, tile_step, 0)

            @pl.when((i > 0) & (slot == 3))
            def _():
                m1(i - 1)
            return c2
        lax.fori_loop(1, n_cp, slot_step, 0)
        for kv in range(kv_n):
            inv = 1.0 / l_st[kv]
            for g in range(groups):
                lanes = slice(g * QC, (g + 1) * QC)
                h = kv * groups + g
                orow[:, h * HEAD_DIM:(h + 1) * HEAD_DIM] = (acc[kv, :, lanes] * inv[:, lanes]).astype(bf16).T

        @pl.when(i == 0)
        def _():
            wo_load.wait()
        p = lax.rem(i, 2)

        def out_step(j, c2):
            cols = pl.ds(pl.multiple_of(j * OUT_COLS, OUT_COLS), OUT_COLS)
            part[p, :, :, cols] = jnp.dot(orow[...], nbuf[:, cols], preferred_element_type=f32).astype(bf16).reshape(n_tp, R, OUT_COLS)
            return c2
        lax.fori_loop(0, D // OUT_COLS, out_step, 0)
        m0(i)

        @pl.when(i > 0)
        def _():
            h_load(i - 1).wait()
            m2(i - 1)
        return carry
    lax.fori_loop(0, Q_CHUNKS, chunk, 0)
    last = Q_CHUNKS - 1
    m1(last)
    h_load(last).wait()
    m2(last)
    for k in range(6):
        kx(k).wait_send()
    for rel in range(n_cp // 2):
        for b in range(2):
            sb(rel, b).wait_send()
    pltpu.make_async_copy(knat, k_out, kvo_sem.at[0]).wait()
    pltpu.make_async_copy(vnat, v_out, kvo_sem.at[1]).wait()
    for i in range(Q_CHUNKS):
        for c in o_store(i):
            c.wait()


def fused_attention(x, attn_gain, mlp_gain, cos2, sin2, w_q, w_k, w_v, w_o, n_tp, n_cp):
    tok, D = x.shape
    kv_n = w_k.shape[1] // HEAD_DIM
    groups = w_q.shape[1] // w_k.shape[1]
    QC = tok // Q_CHUNKS
    QL = QC * groups
    R = QC // n_tp
    H = R // 2
    bf, f32 = jnp.bfloat16, jnp.float32
    anys = pl.BlockSpec(memory_space=pl.ANY)
    vm = pl.BlockSpec(memory_space=pltpu.VMEM)
    own = tok // n_tp
    dma = pltpu.SemaphoreType.DMA
    return pl.pallas_call(
        functools.partial(attn_kernel, n_tp, n_cp),
        out_shape=(jax.ShapeDtypeStruct((tok, kv_n * HEAD_DIM), bf), jax.ShapeDtypeStruct((tok, kv_n * HEAD_DIM), bf),
                   jax.ShapeDtypeStruct((own, D), bf), jax.ShapeDtypeStruct((own, D), bf)),
        in_specs=[anys, vm, vm, vm, vm, anys, anys, anys, anys],
        out_specs=(anys,) * 4,
        scratch_shapes=[
            pltpu.VMEM((tok, D), bf),
            pltpu.VMEM((2, D, PROJ_TILE), bf),
            pltpu.VMEM((n_cp // 2, 2, kv_n, tok, HEAD_DIM), bf),
            pltpu.VMEM((n_cp // 2, 2, kv_n, HEAD_DIM, tok), bf),
            pltpu.VMEM((Q_CHUNKS, kv_n, HEAD_DIM, QL), bf),
            pltpu.VMEM((2, n_tp, R, D), bf),
            pltpu.VMEM((Q_CHUNKS, 2, H, D), bf),
            pltpu.VMEM((Q_CHUNKS, 2, R, D), bf),
            pltpu.VMEM((Q_CHUNKS, R, D), bf),
            pltpu.VMEM((Q_CHUNKS, R, D), bf),
            pltpu.VMEM((QC, kv_n * groups * HEAD_DIM), bf),
            pltpu.VMEM((kv_n, HEAD_DIM, QL), f32),
            pltpu.VMEM((kv_n, 1, QL), f32),
            pltpu.VMEM((kv_n, 1, QL), f32),
            pltpu.VMEM((tok, kv_n * HEAD_DIM), bf),
            pltpu.VMEM((tok, kv_n * HEAD_DIM), bf),
            dma((Q_CHUNKS,)), dma((2,)), dma, dma((Q_CHUNKS,)), dma((2, Q_CHUNKS)), dma((2,)),
            dma((6,)), dma((6,)), dma((n_cp // 2, 2)), dma((n_cp // 2, 2)), dma((Q_CHUNKS, 6)), dma((Q_CHUNKS, 6)),
        ],
        compiler_params=pltpu.CompilerParams(collective_id=1, has_side_effects=True, vmem_limit_bytes=VMEM_LIMIT),
        name='fused_attention',
    )(x, attn_gain.reshape(1, D), mlp_gain.reshape(1, D), cos2, sin2, w_q, w_k, w_v, w_o)


def mlp_kernel(n_tp, n_hbm, h_ref, wg_hbm, wu_hbm, wd_hbm, out_hbm,
               nbuf, act, wg_buf, wu_buf, wd_buf, part, relay, fin, xfin,
               wsem, dsem, own_sem, ag_send, ag_recv, rs_send, rs_recv, go_send, go_recv, loc_sem):
    me = lax.axis_index('tp')
    right = lax.rem(me + 1, n_tp)
    left = lax.rem(me + n_tp - 1, n_tp)
    _, _, R, D = nbuf.shape
    H = R // 2
    DG = part.shape[-1]
    n_ff = act.shape[1] // FF_TILE
    n_out = D // OUT_TILE
    per_group = DG // OUT_TILE
    lo, hi = pl.ds(0, H), pl.ds(H, H)

    def remote(src, dst, ssem, rsem, to):
        return pltpu.make_async_remote_copy(src_ref=src, dst_ref=dst, send_sem=ssem, recv_sem=rsem,
                                            device_id={'tp': to}, device_id_type=pl.DeviceIdType.MESH)

    def ag(s, k):
        src_slot, dst_slot, rows, to = ((0, 1, lo, right), (0, 1, hi, right), (0, 2, hi, left), (0, 2, lo, left),
                                        (1, 3, lo, right), (2, 3, hi, left))[k]
        return remote(nbuf.at[s, src_slot, rows], nbuf.at[s, dst_slot, rows], ag_send.at[s, k], ag_recv.at[s, k], to)

    def rs(s, g, k):
        src, dst, to = ((part.at[s, g, 3, lo], relay.at[s, g, 0], right),
                        (part.at[s, g, 3, hi], relay.at[s, g, 1], left),
                        (part.at[s, g, 2, hi], fin.at[s, g, 0, hi], right),
                        (part.at[s, g, 1, lo], fin.at[s, g, 1, lo], left),
                        (part.at[s, g, 2, lo], fin.at[s, g, 0, lo], right),
                        (part.at[s, g, 1, hi], fin.at[s, g, 1, hi], left))[k]
        return remote(src, dst, rs_send.at[s, g, k], rs_recv.at[s, g, k], to)

    def out_rows(owner, s, half):
        return pl.ds(pl.multiple_of(((HALVES * s + half) * n_tp + owner) * H, H), H)

    def go(s, g, k):
        cols = pl.ds(g * DG, DG)
        half = (0, 1, 1, 0, 0, 1)[k]
        to = (right, right, left, left, right, left)[k]
        owner = (me, me, me, me, left, right)[k]
        dst = out_hbm.at[out_rows(owner, s, half), cols]
        src = xfin.at[s, g, pl.ds(half * H, H)] if k < 4 else dst
        return remote(src, dst, go_send.at[s, g, k], go_recv.at[s, g, k], to)

    def loc(s, g, half):
        return pltpu.make_async_copy(xfin.at[s, g, pl.ds(half * H, H)], out_hbm.at[out_rows(me, s, half), pl.ds(g * DG, DG)],
                                     loc_sem.at[s, g, half])

    def own(s):
        return pltpu.make_async_copy(n_hbm.at[pl.ds(s * R, R)], nbuf.at[s, 0], own_sem.at[s])

    def gu_load(t, slot):
        cols = pl.ds(pl.multiple_of(t * FF_TILE, FF_TILE), FF_TILE)
        return (pltpu.make_async_copy(wg_hbm.at[:, cols], wg_buf.at[slot], wsem.at[0, slot]),
                pltpu.make_async_copy(wu_hbm.at[:, cols], wu_buf.at[slot], wsem.at[1, slot]))

    def dn_load(j, slot):
        cols = pl.ds(pl.multiple_of(j * OUT_TILE, OUT_TILE), OUT_TILE)
        return pltpu.make_async_copy(wd_hbm.at[:, cols], wd_buf.at[slot], dsem.at[slot])

    def gu_first():
        for t in range(2):
            for c in gu_load(t, t):
                c.start()

    def dn_first():
        for j in range(2):
            dn_load(j, j).start()

    for s in range(HALVES):
        own(s).start()
    gu_first()
    dn_first()
    barrier = pltpu.get_barrier_semaphore()
    for nbr in (left, right):
        pl.semaphore_signal(barrier, inc=1, device_id={'tp': nbr}, device_id_type=pl.DeviceIdType.MESH)
    pl.semaphore_wait(barrier, 2)

    def ag_own(s):
        own(s).wait()
        for k in range(4):
            ag(s, k).start()

    def ag_fwd(s, k):
        ag(s, k).wait_recv()
        ag(s, 4 + k // 2).start()

    def ag_rest(s):
        for k in (1, 3, 4, 5):
            ag(s, k).wait_recv()

    def m0(s, g):
        for k in range(4):
            rs(s, g, k).start()

    def m1(s, g):
        for i, slot, rows in ((0, 2, lo), (1, 1, hi)):
            rs(s, g, i).wait_recv()
            total = part[s, g, slot, rows, :].astype(jnp.float32) + relay[s, g, i].astype(jnp.float32)
            part[s, g, slot, rows, :] = total.astype(jnp.bfloat16)
        rs(s, g, 4).start()
        rs(s, g, 5).start()

    def m2(s, g):
        for k in range(2, 6):
            rs(s, g, k).wait_recv()
        total = (part[s, g, 0].astype(jnp.float32) + fin[s, g, 0].astype(jnp.float32)) + fin[s, g, 1].astype(jnp.float32)
        res = h_ref[pl.ds(s * R, R), pl.ds(g * DG, DG)].astype(jnp.float32)
        xfin[s, g] = (res + total).astype(jnp.bfloat16)
        for k in range(4):
            go(s, g, k).start()
        for half in range(2):
            loc(s, g, half).start()

    def m3(s, g):
        go(s, g, 0).wait_recv()
        go(s, g, 4).start()
        go(s, g, 2).wait_recv()
        go(s, g, 5).start()

    def gate_up(s, hooks):
        def step(t, carry):
            slot = lax.rem(t, 2)
            for c in gu_load(t, slot):
                c.wait()
            rows = nbuf[s].reshape(4 * R, D)
            gate = jnp.dot(rows, wg_buf[slot], preferred_element_type=jnp.float32)
            up = jnp.dot(rows, wu_buf[slot], preferred_element_type=jnp.float32)
            act[:, pl.ds(pl.multiple_of(t * FF_TILE, FF_TILE), FF_TILE)] = (jax.nn.silu(gate) * up).astype(jnp.bfloat16)

            @pl.when(t + 2 < n_ff)
            def _():
                for c in gu_load(t + 2, slot):
                    c.start()
            for at, fn in hooks:
                pl.when(t == at)(fn)
            return carry
        lax.fori_loop(0, n_ff, step, 0)

    def down(s, hooks):
        def step(j, carry):
            slot = lax.rem(j, 2)
            dn_load(j, slot).wait()
            res = jnp.dot(act[...], wd_buf[slot], preferred_element_type=jnp.float32).astype(jnp.bfloat16)
            g, c = j // per_group, lax.rem(j, per_group)
            part[s, g, :, :, pl.ds(pl.multiple_of(c * OUT_TILE, OUT_TILE), OUT_TILE)] = res.reshape(4, R, OUT_TILE)

            @pl.when(j + 2 < n_out)
            def _():
                dn_load(j + 2, slot).start()
            for at, fn in hooks:
                pl.when(j == at)(fn)
            return carry
        lax.fori_loop(0, n_out, step, 0)

    P_ = functools.partial
    G = GROUPS_OUT
    ag_own(0)
    ag_fwd(0, 0)
    ag_fwd(0, 2)
    ag_own(1)
    ag_rest(0)
    gate_up(0, [(6, P_(ag_fwd, 1, 0)), (7, P_(ag_fwd, 1, 2))])
    gu_first()
    send_hooks = lambda s: [(per_group * (g + 1), P_(m0, s, g)) for g in range(G - 1)]
    down(0, send_hooks(0) + [(13, P_(m1, 0, 0)), (18, P_(m1, 0, 1))])
    m0(0, G - 1)
    dn_first()
    ag_rest(1)
    gate_up(1, [(1, P_(m1, 0, 2)), (4, P_(m1, 0, 3))] + [(6 + 2 * g, P_(m2, 0, g)) for g in range(G)])
    down(1, send_hooks(1) + [(per_group * g + 2, P_(m3, 0, g)) for g in range(G)] + [(13, P_(m1, 1, 0)), (18, P_(m1, 1, 1))])
    m0(1, G - 1)
    m1(1, 2)
    m1(1, 3)
    m2(1, 0)
    m2(1, 1)
    m3(1, 0)
    m2(1, 2)
    m3(1, 1)
    m2(1, 3)
    m3(1, 2)
    m3(1, 3)
    for s in range(HALVES):
        for k in range(6):
            ag(s, k).wait_send()
        for g in range(G):
            for half in range(2):
                loc(s, g, half).wait()
            for k in range(6):
                rs(s, g, k).wait_send()
                go(s, g, k).wait_send()
            for k in (1, 3, 4, 5):
                go(s, g, k).wait_recv()


def fused_mlp(normed, hidden, w_gate, w_up, w_down, n_tp):
    own_rows, D = normed.shape
    F = w_gate.shape[1]
    R = own_rows // HALVES
    H = R // 2
    DG = D // GROUPS_OUT
    bf = jnp.bfloat16
    S, G = HALVES, GROUPS_OUT
    anys = pl.BlockSpec(memory_space=pl.ANY)
    vm = pl.BlockSpec(memory_space=pltpu.VMEM)
    return pl.pallas_call(
        functools.partial(mlp_kernel, n_tp),
        out_shape=jax.ShapeDtypeStruct((own_rows * n_tp, D), bf),
        in_specs=[anys, vm, anys, anys, anys],
        out_specs=anys,
        scratch_shapes=[
            pltpu.VMEM((S, 4, R, D), bf),
            pltpu.VMEM((4 * R, F), bf),
            pltpu.VMEM((2, D, FF_TILE), bf),
            pltpu.VMEM((2, D, FF_TILE), bf),
            pltpu.VMEM((2, F, OUT_TILE), bf),
            pltpu.VMEM((S, G, 4, R, DG), bf),
            pltpu.VMEM((S, G, 2, H, DG), bf),
            pltpu.VMEM((S, G, 2, R, DG), bf),
            pltpu.VMEM((S, G, R, DG), bf),
            pltpu.SemaphoreType.DMA((2, 2)),
            pltpu.SemaphoreType.DMA((2,)),
            pltpu.SemaphoreType.DMA((S,)),
            pltpu.SemaphoreType.DMA((S, 6)),
            pltpu.SemaphoreType.DMA((S, 6)),
            pltpu.SemaphoreType.DMA((S, G, 6)),
            pltpu.SemaphoreType.DMA((S, G, 6)),
            pltpu.SemaphoreType.DMA((S, G, 6)),
            pltpu.SemaphoreType.DMA((S, G, 6)),
            pltpu.SemaphoreType.DMA((S, G, 2)),
        ],
        compiler_params=pltpu.CompilerParams(collective_id=0, has_side_effects=True, vmem_limit_bytes=VMEM_LIMIT),
        cost_estimate=pl.CostEstimate(flops=2 * own_rows * n_tp * D * F * 3, bytes_accessed=2 * 3 * 2 * D * F, transcendentals=0),
        name='fused_mlp',
    )(normed, hidden, w_gate, w_up, w_down)


def rope_tables(positions):
    inv_freq = jnp.asarray(ROPE_THETA, jnp.float32) ** (-jnp.arange(0, HEAD_DIM, 2, dtype=jnp.float32) / HEAD_DIM)
    angles = positions.astype(jnp.float32)[:, None] * inv_freq[None, :]
    return jnp.cos(angles), jnp.sin(angles)


def solution(mesh):
    n_tp, n_cp = mesh.shape['tp'], mesh.shape['cp']
    row_spec = P(('dp', 'cp'), None)
    cache_spec = P(('dp', 'cp'), 'tp', None)
    col_spec = P(None, 'tp')
    split_rows = P('tp', None)
    vec_spec = P(None)

    def local_layer(x, attn_gain, w_q, w_k, w_v, w_o, mlp_gain, w_gate, w_up, w_down):
        tok_dev = x.shape[0]
        kv_local = w_k.shape[1] // HEAD_DIM
        cos_tab, sin_tab = rope_tables(lax.axis_index('cp') * tok_dev + jnp.arange(tok_dev))
        cos2 = jnp.concatenate([cos_tab, cos_tab], axis=-1)
        sin2 = jnp.concatenate([-sin_tab, sin_tab], axis=-1)
        keys, values, hidden, normed = fused_attention(x, attn_gain, mlp_gain, cos2, sin2, w_q, w_k, w_v, w_o, n_tp, n_cp)
        x_out = fused_mlp(normed, hidden, w_gate, w_up, w_down, n_tp)
        return x_out, keys.reshape(tok_dev, kv_local, HEAD_DIM), values.reshape(tok_dev, kv_local, HEAD_DIM)

    return jax.shard_map(local_layer, mesh=mesh,
                         in_specs=(row_spec, vec_spec, col_spec, col_spec, col_spec, split_rows, vec_spec, col_spec, col_spec, split_rows),
                         out_specs=(row_spec, cache_spec, cache_spec), check_vma=False)
```

```python
import functools
import math
import jax
import jax.numpy as jnp
from jax import lax
from jax.experimental import pallas as pl
from jax.experimental.pallas import tpu as pltpu
from jax.sharding import PartitionSpec as P

HEAD_DIM = 128
OWN, LEFT, RIGHT, FAR = SLOTS = range(4)
LO, HI = BOTH = range(2)
KEY, VALUE = BOTH
KV_A, KV_B = BOTH
ROPE_THETA = 1000000.0
NORM_EPS = 1e-5
MASK_VALUE = -1e30
VMEM_LIMIT = 66000000
HALVES = 2
GROUPS_OUT = 4
COPY_BLOCKS = 16
FF_TILE = 256
OUT_TILE = 256
DN_BUFS = 3
PROJ_TILE = 256
Q_CHUNKS = 4
OUT_COLS = 2560
NORM_ROWS = 16
ANGLE_ROWS = 32


def attn_kernel(n_tp, n_cp, x_hbm, gain_ref, mlp_gain_ref, freq_ref, wq_hbm, wk_hbm, wv_hbm, wo_hbm,
                k_out, v_out, h_out, n_out,
                nbuf, wt, kbuf, vbuf, qt, part, relay, fin, hrow, nrow, orow, s0, s1, acc, m_st, l_st, cos_s, sin_s, bias, vnat, cache,
                xsem, wsem, wosem, hsem, osem, kvo_sem, kx_send, kx_recv, sb_send, sb_recv, rs_send, rs_recv):
    tok, D = nbuf.shape
    kv_n, HT = kbuf.shape[3], kbuf.shape[4]
    QC = tok // Q_CHUNKS
    QL = qt.shape[3]
    groups = QL // QC
    R = QC // n_tp
    H = R // 2
    lo, hi = pl.ds(0, H), pl.ds(H, H)
    me = lax.axis_index('tp')
    right = lax.rem(me + 1, n_tp)
    left = lax.rem(me + n_tp - 1, n_tp)
    far = lax.rem(me + 2, n_tp)
    cp = lax.axis_index('cp')
    core = lax.rem(cp, 2)
    chip = cp // 2
    last_chip = n_cp // 2 - 1
    sib = cp + 1 - 2 * core
    x_right = lax.rem(cp + 2, n_cp)
    x_left = lax.rem(cp + n_cp - 2, n_cp)
    cexp = (HEAD_DIM ** -0.5) * math.log2(math.e)
    f32, bf16 = jnp.float32, jnp.bfloat16
    s_buf = (s0, s1)

    def remote(src, dst, ssem, rsem, to):
        return pltpu.make_async_remote_copy(src_ref=src, dst_ref=dst, send_sem=ssem, recv_sem=rsem,
                                            device_id=to, device_id_type=pl.DeviceIdType.MESH)

    def kx(k, b):
        buf = (kbuf, vbuf)[b]
        src, dst, half, to = ((OWN, LEFT, LO, x_right), (OWN, LEFT, HI, x_right), (OWN, RIGHT, LO, x_left), (OWN, RIGHT, HI, x_left),
                              (LEFT, FAR, LO, x_right), (RIGHT, FAR, HI, x_left))[k]
        return remote(buf.at[src, LO, half], buf.at[dst, LO, half], kx_send.at[k, b], kx_recv.at[k, b], {'cp': to})

    def sb(rel, half, b):
        buf = (kbuf, vbuf)[b]
        return remote(buf.at[rel, LO, half], buf.at[rel, HI, half], sb_send.at[rel, half, b], sb_recv.at[rel, half, b], {'cp': sib})

    def rs(i, k):
        p = lax.rem(i, 2)
        src, dst, to = ((part.at[p, far, lo], relay.at[i, LO], right),
                        (part.at[p, far, hi], relay.at[i, HI], left),
                        (part.at[p, right, hi], fin.at[i, LO, hi], right),
                        (part.at[p, left, lo], fin.at[i, HI, lo], left),
                        (part.at[p, right, lo], fin.at[i, LO, lo], right),
                        (part.at[p, left, hi], fin.at[i, HI, hi], left))[k]
        return remote(src, dst, rs_send.at[i, k], rs_recv.at[i, k], {'tp': to})

    def x_load(c):
        rows = pl.ds(pl.multiple_of(c * QC, QC), QC)
        return pltpu.make_async_copy(x_hbm.at[rows], nbuf.at[rows], xsem.at[c])

    def w_load(ref, t, slot):
        return pltpu.make_async_copy(ref.at[:, pl.ds(pl.multiple_of(t * PROJ_TILE, PROJ_TILE), PROJ_TILE)], wt.at[slot], wsem.at[slot])

    def h_load(i):
        return pltpu.make_async_copy(x_hbm.at[pl.ds(pl.multiple_of(i * QC + me * R, R), R)], hrow.at[i], hsem.at[i])

    def o_store(i):
        rows = pl.ds(i * R, R)
        return (pltpu.make_async_copy(hrow.at[i], h_out.at[rows], osem.at[0, i]),
                pltpu.make_async_copy(nrow.at[i], n_out.at[rows], osem.at[1, i]))

    wo_load = pltpu.make_async_copy(wo_hbm, nbuf, wosem)

    x_load(0).start()
    barrier = pltpu.get_barrier_semaphore()
    for to in ({'tp': left}, {'tp': right}, {'cp': x_left}, {'cp': x_right}, {'cp': sib}):
        pl.semaphore_signal(barrier, inc=1, device_id=to, device_id_type=pl.DeviceIdType.MESH)

    def make_tables():
        freq = freq_ref[...]

        def angles(step, base):
            t = lax.broadcasted_iota(jnp.int32, (ANGLE_ROWS, HEAD_DIM), 0) * step + base
            a = t.astype(f32) * freq
            return jnp.cos(a), jnp.sin(a)

        sign = jnp.where(lax.broadcasted_iota(jnp.int32, (1, HEAD_DIM), 1) < HEAD_DIM // 2, -1.0, 1.0)
        fine_cos, fine_sin = angles(1, 0)
        base_cos, base_sin = angles(ANGLE_ROWS, cp * tok)
        for b in range(tok // ANGLE_ROWS):
            ca, sa = base_cos[b:b + 1], base_sin[b:b + 1]
            rows = slice(b * ANGLE_ROWS, (b + 1) * ANGLE_ROWS)
            cos_s[rows, :] = ca * fine_cos - sa * fine_sin
            sin_s[rows, :] = (sa * fine_cos + ca * fine_sin) * sign

    def make_bias():
        key_at = lax.broadcasted_iota(jnp.int32, bias.shape[1:], 0)
        row_at = lax.broadcasted_iota(jnp.int32, bias.shape[1:], 1)
        for odd in BOTH:
            bias[odd] = jnp.where(key_at <= row_at + odd * QC, 0.0, MASK_VALUE)

    def normalize(wide, gain):
        inv = lax.rsqrt(jnp.mean(wide * wide, axis=-1, keepdims=True) + NORM_EPS)
        return (wide * inv * gain).astype(bf16)

    gain = gain_ref[...].astype(f32)[None, :]

    def stage(c):
        return nrow if c % 2 == 0 else part.at[0]

    def inv_rows(c, b):
        first = (c % 2) * QC + b * NORM_ROWS
        return slice(first, first + NORM_ROWS)

    def stat_chunk(c):
        for b in range(QC // NORM_ROWS):
            rows = slice(c * QC + b * NORM_ROWS, c * QC + (b + 1) * NORM_ROWS)
            wide = nbuf[rows, :].astype(f32)
            s0[inv_rows(c, b), 0:1] = lax.rsqrt(jnp.mean(wide * wide, axis=-1, keepdims=True) + NORM_EPS)

    def norm_chunk(c):
        for b in range(QC // NORM_ROWS):
            rows = slice(c * QC + b * NORM_ROWS, c * QC + (b + 1) * NORM_ROWS)
            scaled = (nbuf[rows, :].astype(f32) * s0[inv_rows(c, b), 0:1] * gain).astype(bf16)
            nbuf[rows, :] = scaled
            stage(c)[b * NORM_ROWS // R, b * NORM_ROWS % R:b * NORM_ROWS % R + NORM_ROWS, :] = scaled

    def rope(u, rows, scale=None):
        wide = u.astype(bf16).astype(f32)
        turned = wide * cos_s[rows, :] + pltpu.roll(wide, HEAD_DIM // 2, 1) * sin_s[rows, :]
        return (turned if scale is None else turned * scale).astype(bf16)

    x_load(0).wait()
    w_load(wk_hbm, 0, 0).start()
    w_load(wv_hbm, 0, 1).start()
    x_load(1).start()
    stat_chunk(0)
    norm_chunk(0)
    x_load(1).wait()
    x_load(2).start()
    x_load(3).start()
    stat_chunk(1)
    w_load(wk_hbm, 0, 0).wait()
    w_load(wv_hbm, 0, 1).wait()
    w_load(wq_hbm, 0, 2).start()
    for i in range(Q_CHUNKS):
        h_load(i).start()
    for c in range(Q_CHUNKS):
        rows = slice(c * QC, (c + 1) * QC)
        half = c // 2
        part_rows = slice((c % 2) * QC, (c % 2 + 1) * QC)
        if c + 2 < Q_CHUNKS:
            x_load(c + 2).wait()
        n_rows = stage(c)[...].reshape(QC, D)
        k_res = jnp.dot(n_rows, wt[0], preferred_element_type=f32)
        v_res = jnp.dot(n_rows, wt[1], preferred_element_type=f32).astype(bf16)
        if c == 0:
            make_tables()
        if c == Q_CHUNKS - 1:
            make_bias()
        if c + 1 < Q_CHUNKS:
            norm_chunk(c + 1)
        if c + 2 < Q_CHUNKS:
            stat_chunk(c + 2)
        vnat[rows, :] = v_res
        for j in range(kv_n):
            cols = slice(j * HEAD_DIM, (j + 1) * HEAD_DIM)
            head = rope(k_res[:, cols], rows)
            kbuf[OWN, LO, half, j, part_rows, :] = head
            vbuf[OWN, LO, half, j, :, part_rows] = v_res[:, cols].T
        if c == 1:
            pl.semaphore_wait(barrier, 5)
            for b in BOTH:
                kx(OWN, b).start()
                kx(2, b).start()
                sb(OWN, LO, b).start()
    w_load(wq_hbm, 1, 0).start()
    w_load(wq_hbm, 2, 1).start()
    for b in BOTH:
        kx(1, b).start()
        kx(3, b).start()
        sb(OWN, HI, b).start()

    n_q = wq_hbm.shape[1] // PROJ_TILE
    heads_tile = PROJ_TILE // HEAD_DIM
    tiles_kv = n_q // kv_n

    def q_step(t, carry):
        slot = lax.rem(t + 2, 3)
        w_load(wq_hbm, t, slot).wait()
        res = jnp.dot(nbuf[...], wt[slot], preferred_element_type=f32)
        kv, base = t // tiles_kv, lax.rem(t, tiles_kv) * heads_tile
        for j in range(heads_tile):
            head = rope(res[:, j * HEAD_DIM:(j + 1) * HEAD_DIM], slice(None), cexp)
            lanes = pl.ds(pl.multiple_of((base + j) * QC, QC), QC)
            for i in range(Q_CHUNKS):
                qt[i, kv, :, lanes] = head[i * QC:(i + 1) * QC].T

        @pl.when(t + 3 < n_q)
        def _():
            w_load(wq_hbm, t + 3, slot).start()
        return carry
    lax.fori_loop(0, n_q, q_step, 0)
    wo_load.start()
    for b in BOTH:
        kx(OWN, b).wait_recv()
        kx(4, b).start()
        sb(LEFT, LO, b).start()
        kx(2, b).wait_recv()
        sb(RIGHT, LO, b).start()
    for half in BOTH:
        for b in BOTH:
            sb(OWN, half, b).wait_recv()

    def ev_near():
        for b in BOTH:
            kx(1, b).wait_recv()
            sb(LEFT, HI, b).start()
            kx(3, b).wait_recv()
            kx(5, b).start()
            sb(RIGHT, HI, b).start()

    def ev_far():
        for b in BOTH:
            kx(4, b).wait_recv()
            sb(FAR, LO, b).start()
            kx(5, b).wait_recv()
            sb(FAR, HI, b).start()

    def ev_sib(rel):
        for half in BOTH:
            for b in BOTH:
                sb(rel, half, b).wait_recv()

    n_far = core + jnp.where(chip >= 1, 2, 0) + jnp.where(chip == last_chip, 2, 0)
    events = ((ev_near, core), (functools.partial(ev_sib, LEFT), core + 1),
              (functools.partial(ev_sib, RIGHT), jnp.where(chip == last_chip, core + 3, n_cp)),
              (ev_far, n_far), (functools.partial(ev_sib, FAR), n_far + 1))

    def block_of(n):
        own = n >= cp
        sib_block = (core == 1) & (n == 0)
        p = n - core
        pair = p // 2
        rel = jnp.where(own | sib_block, OWN, jnp.where(pair == OWN, LEFT, jnp.where(chip == last_chip, pair + 1, FAR)))
        which = jnp.where(own, LO, jnp.where(sib_block, HI, lax.rem(p + 2, 2)))
        return rel, which

    def scores(i, kv, tile, half):
        rel, which = tile
        s_buf[kv][...] = jnp.dot(kbuf[rel, which, half, kv], qt[i, kv], preferred_element_type=f32)

    def soft(kv, tile, half, off=None):
        first = off is not None
        rel, which = tile
        s = s_buf[kv][...]
        if first:
            s = s + jnp.concatenate([bias[off]] * groups, axis=1)
        m_new = jnp.max(s, axis=0, keepdims=True)
        if not first:
            m_old = m_st[kv]
            m_new = jnp.maximum(m_old, m_new)
            alpha = jnp.exp2(m_old - m_new)
        p = jnp.exp2(s - m_new)
        total = jnp.sum(p, axis=0, keepdims=True)
        add = jnp.dot(vbuf[rel, which, half, kv], p.astype(bf16), preferred_element_type=f32)
        m_st[kv] = m_new
        if first:
            l_st[kv] = total
            acc[kv] = add
        else:
            l_st[kv] = l_st[kv] * alpha + total
            acc[kv] = acc[kv] * alpha + add

    def m0(i):
        for k in range(4):
            rs(i, k).start()

    def m1(i):
        p = lax.rem(i, 2)
        for j, owner, rows in ((LO, right, lo), (HI, left, hi)):
            rs(i, j).wait_recv()
            part[p, owner, rows, :] = (part[p, owner, rows, :].astype(f32) + relay[i, j].astype(f32)).astype(bf16)
        rs(i, 4).start()
        rs(i, 5).start()

    mlp_gain = mlp_gain_ref[...].astype(f32)[None, :]

    def m2(i):
        p = lax.rem(i, 2)
        for k in range(2, 6):
            rs(i, k).wait_recv()
        for k in range(6):
            rs(i, k).wait_send()
        total = part[p, me].astype(f32) + fin[i, LO].astype(f32) + fin[i, HI].astype(f32)
        hid = (hrow[i].astype(f32) + total).astype(bf16)
        hrow[i] = hid
        nrow[i] = normalize(hid.astype(f32), mlp_gain)
        for c in o_store(i):
            c.start()

    def chunk(i, carry):
        first, later, before = i == 0, i > 0, i - 1
        def fire(block):
            for fn, at in events:
                @pl.when(first & (at < cp) & (block == at))
                def _():
                    fn()
        own = (0, 0)
        fire(0)
        first_block = block_of(0)
        off = lax.rem(i, 2)
        late = i // 2

        def diag_step(_, c2):
            scores(i, KV_A, own, late)
            scores(i, KV_B, own, late)
            soft(KV_A, own, late, off)
            scores(i, KV_A, (jnp.where(late == 1, 0, first_block[0]), jnp.where(late == 1, 0, first_block[1])), 0)
            soft(KV_B, own, late, off)
            return c2
        lax.fori_loop(0, 1, diag_step, 0)

        def own_step(_, c2):
            scores(i, KV_B, own, LO)
            soft(KV_A, own, LO)
            scores(i, KV_A, first_block, LO)
            soft(KV_B, own, LO)
            return c2
        lax.fori_loop(0, late, own_step, 0)

        def pair_step(n, c2):
            fire(n + 1)

            @pl.when(later & (n == cp // 2))
            def _():
                m1(before)
            blk = block_of(n)
            scores(i, KV_B, blk, LO)
            soft(KV_A, blk, LO)
            scores(i, KV_A, blk, HI)
            soft(KV_B, blk, LO)
            scores(i, KV_B, blk, HI)
            soft(KV_A, blk, HI)
            scores(i, KV_A, block_of(n + 1), LO)
            soft(KV_B, blk, HI)
            return c2
        lax.fori_loop(0, cp, pair_step, 0)

        @pl.when(first)
        def _():
            for fn, at in events:
                pl.when(at >= cp)(fn)
            wo_load.wait()

        @pl.when(later & (cp == 0))
        def _():
            m1(before)
        for kv in range(kv_n):
            inv = 1.0 / l_st[kv]
            for g in range(groups):
                lanes = slice(g * QC, (g + 1) * QC)
                h = kv * groups + g
                orow[:, h * HEAD_DIM:(h + 1) * HEAD_DIM] = (acc[kv, :, lanes] * inv[:, lanes]).astype(bf16).T
        p = lax.rem(i, 2)

        def out_step(j, c2):
            cols = pl.ds(pl.multiple_of(j * OUT_COLS, OUT_COLS), OUT_COLS)
            part[p, :, :, cols] = jnp.dot(orow[...], nbuf[:, cols], preferred_element_type=f32).astype(bf16).reshape(n_tp, R, OUT_COLS)
            return c2
        lax.fori_loop(0, D // OUT_COLS, out_step, 0)
        m0(i)

        @pl.when(later)
        def _():
            h_load(before).wait()
            m2(before)
        return carry
    lax.fori_loop(0, Q_CHUNKS, chunk, 0)
    last = Q_CHUNKS - 1
    for n, out in enumerate((k_out, v_out)):
        for j in range(kv_n):
            if n:
                cache[:, j, :] = vnat[:, j * HEAD_DIM:(j + 1) * HEAD_DIM]
            else:
                for half in BOTH:
                    cache[half * HT:(half + 1) * HT, j, :] = kbuf[OWN, LO, half, j]
        stored = pltpu.make_async_copy(cache, out, kvo_sem.at[n])
        stored.start()
        stored.wait()
    m1(last)
    h_load(last).wait()
    m2(last)
    for b in BOTH:
        for k in range(6):
            kx(k, b).wait_send()
        for rel in range(n_cp // 2):
            for half in BOTH:
                sb(rel, half, b).wait_send()
    for i in range(Q_CHUNKS):
        for c in o_store(i):
            c.wait()


def fused_attention(x, attn_gain, mlp_gain, w_q, w_k, w_v, w_o, n_tp, n_cp):
    tok, D = x.shape
    kv_n = w_k.shape[1] // HEAD_DIM
    groups = w_q.shape[1] // w_k.shape[1]
    QC = tok // Q_CHUNKS
    QL = QC * groups
    R = QC // n_tp
    H = R // 2
    HT = tok // 2
    bf, f32 = jnp.bfloat16, jnp.float32
    anys = pl.BlockSpec(memory_space=pl.ANY)
    vm = pl.BlockSpec(memory_space=pltpu.VMEM)
    own = tok // n_tp
    dma = pltpu.SemaphoreType.DMA
    inv_freq = jnp.asarray(ROPE_THETA, f32) ** (-jnp.arange(0, HEAD_DIM, 2, dtype=f32) / HEAD_DIM)
    freq = jnp.concatenate([inv_freq, inv_freq]).reshape(1, HEAD_DIM)
    return pl.pallas_call(
        functools.partial(attn_kernel, n_tp, n_cp),
        out_shape=(jax.ShapeDtypeStruct((tok, kv_n, HEAD_DIM), bf), jax.ShapeDtypeStruct((tok, kv_n, HEAD_DIM), bf),
                   jax.ShapeDtypeStruct((own, D), bf), jax.ShapeDtypeStruct((own, D), bf)),
        in_specs=[anys, vm, vm, vm, anys, anys, anys, anys],
        out_specs=(anys,) * 4,
        scratch_shapes=[
            pltpu.VMEM((tok, D), bf),
            pltpu.VMEM((3, D, PROJ_TILE), bf),
            pltpu.VMEM((n_cp // 2, 2, 2, kv_n, HT, HEAD_DIM), bf),
            pltpu.VMEM((n_cp // 2, 2, 2, kv_n, HEAD_DIM, HT), bf),
            pltpu.VMEM((Q_CHUNKS, kv_n, HEAD_DIM, QL), bf),
            pltpu.VMEM((2, n_tp, R, D), bf),
            pltpu.VMEM((Q_CHUNKS, 2, H, D), bf),
            pltpu.VMEM((Q_CHUNKS, 2, R, D), bf),
            pltpu.VMEM((Q_CHUNKS, R, D), bf),
            pltpu.VMEM((Q_CHUNKS, R, D), bf),
            pltpu.VMEM((QC, kv_n * groups * HEAD_DIM), bf),
            pltpu.VMEM((HT, QL), f32),
            pltpu.VMEM((HT, QL), f32),
            pltpu.VMEM((kv_n, HEAD_DIM, QL), f32),
            pltpu.VMEM((kv_n, 1, QL), f32),
            pltpu.VMEM((kv_n, 1, QL), f32),
            pltpu.VMEM((tok, HEAD_DIM), f32),
            pltpu.VMEM((tok, HEAD_DIM), f32),
            pltpu.VMEM((2, HT, QC), f32),
            pltpu.VMEM((tok, kv_n * HEAD_DIM), bf),
            pltpu.VMEM((tok, kv_n, HEAD_DIM), bf),
            dma((Q_CHUNKS,)), dma((3,)), dma, dma((Q_CHUNKS,)), dma((2, Q_CHUNKS)), dma((2,)),
            dma((6, 2)), dma((6, 2)), dma((n_cp // 2, 2, 2)), dma((n_cp // 2, 2, 2)), dma((Q_CHUNKS, 6)), dma((Q_CHUNKS, 6)),
        ],
        compiler_params=pltpu.CompilerParams(collective_id=1, has_side_effects=True, vmem_limit_bytes=VMEM_LIMIT),
        name='fused_attention',
    )(x, attn_gain, mlp_gain, freq, w_q, w_k, w_v, w_o)


def mlp_kernel(n_tp, n_hbm, h_hbm, wg_hbm, wu_hbm, wd_hbm, out_hbm,
               nbuf, act, wg_buf, wu_buf, wd_buf, part, relay, fin, xfin, h_ref,
               h_sem, wsem, dsem, own_sem, ag_send, ag_recv, rs_send, rs_recv, go_send, go_recv, loc_sem):
    me = lax.axis_index('tp')
    right = lax.rem(me + 1, n_tp)
    left = lax.rem(me + n_tp - 1, n_tp)
    _, _, R, D = nbuf.shape
    H = R // 2
    DG = part.shape[-1]
    n_ff = act.shape[1] // FF_TILE
    n_out = D // OUT_TILE
    per_group = DG // OUT_TILE
    lo, hi = pl.ds(0, H), pl.ds(H, H)

    def remote(src, dst, ssem, rsem, to):
        return pltpu.make_async_remote_copy(src_ref=src, dst_ref=dst, send_sem=ssem, recv_sem=rsem,
                                            device_id={'tp': to}, device_id_type=pl.DeviceIdType.MESH)

    def ag(s, k):
        src_slot, dst_slot, rows, to = ((OWN, LEFT, lo, right), (OWN, LEFT, hi, right), (OWN, RIGHT, hi, left), (OWN, RIGHT, lo, left),
                                        (LEFT, FAR, lo, right), (RIGHT, FAR, hi, left))[k]
        return remote(nbuf.at[s, src_slot, rows], nbuf.at[s, dst_slot, rows], ag_send.at[s, k], ag_recv.at[s, k], to)

    def rs(s, g, k):
        src, dst, to = ((part.at[s, g, FAR, lo], relay.at[s, g, LO], right),
                        (part.at[s, g, FAR, hi], relay.at[s, g, HI], left),
                        (part.at[s, g, RIGHT, hi], fin.at[s, g, LO, hi], right),
                        (part.at[s, g, LEFT, lo], fin.at[s, g, HI, lo], left),
                        (part.at[s, g, RIGHT, lo], fin.at[s, g, LO, lo], right),
                        (part.at[s, g, LEFT, hi], fin.at[s, g, HI, hi], left))[k]
        return remote(src, dst, rs_send.at[s, g, k], rs_recv.at[s, g, k], to)

    def out_rows(owner, s, half):
        return pl.ds(pl.multiple_of(((HALVES * s + half) * n_tp + owner) * H, H), H)

    def go(s, g, k):
        cols = pl.ds(g * DG, DG)
        half = (LO, HI, HI, LO, LO, HI)[k]
        to = (right, right, left, left, right, left)[k]
        owner = (me, me, me, me, left, right)[k]
        dst = out_hbm.at[out_rows(owner, s, half), cols]
        src = xfin.at[s, g, pl.ds(half * H, H)] if k < 4 else dst
        return remote(src, dst, go_send.at[s, g, k], go_recv.at[s, g, k], to)

    def loc(s, g, half):
        return pltpu.make_async_copy(xfin.at[s, g, pl.ds(half * H, H)], out_hbm.at[out_rows(me, s, half), pl.ds(g * DG, DG)],
                                     loc_sem.at[s, g, half])

    def own(s):
        return pltpu.make_async_copy(n_hbm.at[pl.ds(s * R, R)], nbuf.at[s, 0], own_sem.at[s])

    def gu_load(t, slot):
        cols = pl.ds(pl.multiple_of(t * FF_TILE, FF_TILE), FF_TILE)
        return (pltpu.make_async_copy(wg_hbm.at[:, cols], wg_buf.at[slot], wsem.at[0, slot]),
                pltpu.make_async_copy(wu_hbm.at[:, cols], wu_buf.at[slot], wsem.at[1, slot]))

    def dn_load(j, slot):
        cols = pl.ds(pl.multiple_of(j * OUT_TILE, OUT_TILE), OUT_TILE)
        return pltpu.make_async_copy(wd_hbm.at[:, cols], wd_buf.at[slot], dsem.at[slot])

    def gu_first():
        for t in range(2):
            for c in gu_load(t, t):
                c.start()

    def dn_first():
        for j in range(DN_BUFS):
            dn_load(j, j).start()

    for s in range(HALVES):
        own(s).start()
    gu_first()
    barrier = pltpu.get_barrier_semaphore()
    for nbr in (left, right):
        pl.semaphore_signal(barrier, inc=1, device_id={'tp': nbr}, device_id_type=pl.DeviceIdType.MESH)
    pl.semaphore_wait(barrier, 2)

    def ag_own(s):
        own(s).wait()
        for k in range(4):
            ag(s, k).start()

    def ag_fwd(s, k):
        ag(s, k).wait_recv()
        ag(s, 4 + k // 2).start()

    def ag_rest(s):
        for k in (1, 3, 4, 5):
            ag(s, k).wait_recv()

    def m0(s, g):
        for k in range(4):
            rs(s, g, k).start()

    def m1(s, g):
        for i, slot, rows in ((LO, RIGHT, lo), (HI, LEFT, hi)):
            rs(s, g, i).wait_recv()
            total = part[s, g, slot, rows, :].astype(jnp.float32) + relay[s, g, i].astype(jnp.float32)
            part[s, g, slot, rows, :] = total.astype(jnp.bfloat16)
        rs(s, g, 4).start()
        rs(s, g, 5).start()

    def m2(s, g):
        for k in range(2, 6):
            rs(s, g, k).wait_recv()
        total = (part[s, g, OWN].astype(jnp.float32) + fin[s, g, LO].astype(jnp.float32)) + fin[s, g, HI].astype(jnp.float32)
        res = h_ref[pl.ds(s * R, R), pl.ds(g * DG, DG)].astype(jnp.float32)
        xfin[s, g] = (res + total).astype(jnp.bfloat16)
        for k in range(4):
            go(s, g, k).start()
        for half in BOTH:
            loc(s, g, half).start()

    def m3(s, g):
        go(s, g, 0).wait_recv()
        go(s, g, 4).start()
        go(s, g, 2).wait_recv()
        go(s, g, 5).start()

    def gate_up(s, first, count, hooks):
        def step(t, carry):
            slot = lax.rem(t, 2)
            for c in gu_load(t, slot):
                c.wait()
            rows = nbuf[s, first:first + count].reshape(count * R, D)
            gate = jnp.dot(rows, wg_buf[slot], preferred_element_type=jnp.float32)
            up = jnp.dot(rows, wu_buf[slot], preferred_element_type=jnp.float32)
            act[first * R:(first + count) * R, pl.ds(pl.multiple_of(t * FF_TILE, FF_TILE), FF_TILE)] = (jax.nn.silu(gate) * up).astype(jnp.bfloat16)

            @pl.when(t + 2 < n_ff)
            def _():
                for c in gu_load(t + 2, slot):
                    c.start()
            for at, fn in hooks:
                pl.when(t == at)(fn)
            return carry
        lax.fori_loop(0, n_ff, step, 0)

    def down(s, hooks):
        def step(j, carry):
            slot = lax.rem(j, DN_BUFS)
            dn_load(j, slot).wait()
            res = jnp.dot(act[...], wd_buf[slot], preferred_element_type=jnp.float32).astype(jnp.bfloat16)
            g, c = j // per_group, lax.rem(j, per_group)
            part[s, g, :, :, pl.ds(pl.multiple_of(c * OUT_TILE, OUT_TILE), OUT_TILE)] = res.reshape(4, R, OUT_TILE)

            @pl.when(j + DN_BUFS < n_out)
            def _():
                dn_load(j + DN_BUFS, slot).start()
            for at, fn in hooks:
                pl.when(j == at)(fn)
            return carry
        lax.fori_loop(0, n_out, step, 0)

    P_ = functools.partial
    G = GROUPS_OUT
    ag_own(0)

    def feed():
        ag_fwd(0, 0)
        ag_fwd(0, 2)
        ag_own(1)
    dn_first()
    h_load = pltpu.make_async_copy(h_hbm, h_ref, h_sem)
    h_load.start()
    gate_up(0, 0, 1, [(7, feed)])
    h_load.wait()
    gu_first()
    ag_rest(0)
    gate_up(0, 1, 3, [(7, P_(ag_fwd, 1, 0)), (8, P_(ag_fwd, 1, 2))])
    gu_first()
    send_hooks = lambda s: [(per_group * (g + 1), P_(m0, s, g)) for g in range(G - 1)]
    down(0, send_hooks(0) + [(13, P_(m1, 0, 0)), (18, P_(m1, 0, 1))])
    m0(0, G - 1)
    dn_first()
    ag_rest(1)
    gate_up(1, 0, 4, [(1, P_(m1, 0, 2)), (4, P_(m1, 0, 3))] + [(6 + 2 * g, P_(m2, 0, g)) for g in range(G)])
    down(1, send_hooks(1) + [(per_group * g + 2, P_(m3, 0, g)) for g in range(G)] + [(13, P_(m1, 1, 0)), (18, P_(m1, 1, 1))])
    m0(1, G - 1)
    m1(1, 2)
    m1(1, 3)
    m2(1, 0)
    m2(1, 1)
    m3(1, 0)
    m2(1, 2)
    m3(1, 1)
    m2(1, 3)
    m3(1, 2)
    m3(1, 3)
    for s in range(HALVES):
        for k in range(6):
            ag(s, k).wait_send()
        for g in range(G):
            for half in BOTH:
                loc(s, g, half).wait()
            for k in range(6):
                rs(s, g, k).wait_send()
                go(s, g, k).wait_send()
            for k in (1, 3, 4, 5):
                go(s, g, k).wait_recv()


def fused_mlp(normed, hidden, w_gate, w_up, w_down, n_tp):
    own_rows, D = normed.shape
    F = w_gate.shape[1]
    R = own_rows // HALVES
    H = R // 2
    DG = D // GROUPS_OUT
    bf = jnp.bfloat16
    S, G = HALVES, GROUPS_OUT
    anys = pl.BlockSpec(memory_space=pl.ANY)
    return pl.pallas_call(
        functools.partial(mlp_kernel, n_tp),
        out_shape=jax.ShapeDtypeStruct((own_rows * n_tp, D), bf),
        in_specs=[anys] * 5,
        out_specs=anys,
        scratch_shapes=[
            pltpu.VMEM((S, 4, R, D), bf),
            pltpu.VMEM((4 * R, F), bf),
            pltpu.VMEM((2, D, FF_TILE), bf),
            pltpu.VMEM((2, D, FF_TILE), bf),
            pltpu.VMEM((DN_BUFS, F, OUT_TILE), bf),
            pltpu.VMEM((S, G, 4, R, DG), bf),
            pltpu.VMEM((S, G, 2, H, DG), bf),
            pltpu.VMEM((S, G, 2, R, DG), bf),
            pltpu.VMEM((S, G, R, DG), bf),
            pltpu.VMEM((own_rows, D), bf),
            pltpu.SemaphoreType.DMA,
            pltpu.SemaphoreType.DMA((2, 2)),
            pltpu.SemaphoreType.DMA((DN_BUFS,)),
            pltpu.SemaphoreType.DMA((S,)),
            pltpu.SemaphoreType.DMA((S, 6)),
            pltpu.SemaphoreType.DMA((S, 6)),
            pltpu.SemaphoreType.DMA((S, G, 6)),
            pltpu.SemaphoreType.DMA((S, G, 6)),
            pltpu.SemaphoreType.DMA((S, G, 6)),
            pltpu.SemaphoreType.DMA((S, G, 6)),
            pltpu.SemaphoreType.DMA((S, G, 2)),
        ],
        compiler_params=pltpu.CompilerParams(collective_id=0, has_side_effects=True, vmem_limit_bytes=VMEM_LIMIT),
        cost_estimate=pl.CostEstimate(flops=2 * own_rows * n_tp * D * F * 3, bytes_accessed=2 * 3 * 2 * D * F, transcendentals=0),
        name='fused_mlp',
    )(normed, hidden, w_gate, w_up, w_down)


def hand_over_kernel(x_in, k_in, v_in, x_out, k_out, v_out, x_buf, k_buf, v_buf, in_sem, out_sem):
    n_blocks, rows, _ = x_buf.shape
    copies = []
    for b in range(n_blocks):
        at = pl.ds(b * rows, rows)
        copies.append((pltpu.make_async_copy(x_in.at[at], x_buf.at[b], in_sem.at[b]), pltpu.make_async_copy(x_buf.at[b], x_out.at[at], out_sem.at[b])))
    for n, (src, buf, dst) in enumerate(((k_in, k_buf, k_out), (v_in, v_buf, v_out))):
        copies.append((pltpu.make_async_copy(src, buf, in_sem.at[n_blocks + n]), pltpu.make_async_copy(buf, dst, out_sem.at[n_blocks + n])))
    for load, _ in copies:
        load.start()
    for load, store in copies:
        load.wait()
        store.start()
    for _, store in copies:
        store.wait()


def hand_over(x_out, keys, values):
    rows, D = x_out.shape
    bf = jnp.bfloat16
    block = rows // COPY_BLOCKS
    anys = pl.BlockSpec(memory_space=pl.ANY)
    dma = pltpu.SemaphoreType.DMA((COPY_BLOCKS + 2,))
    return pl.pallas_call(
        hand_over_kernel,
        out_shape=tuple(jax.ShapeDtypeStruct(a.shape, bf) for a in (x_out, keys, values)),
        in_specs=[anys] * 3,
        out_specs=(anys,) * 3,
        scratch_shapes=[pltpu.VMEM((COPY_BLOCKS, block, D), bf), pltpu.VMEM(keys.shape, bf), pltpu.VMEM(values.shape, bf), dma, dma],
        compiler_params=pltpu.CompilerParams(vmem_limit_bytes=VMEM_LIMIT),
        name='hand_over',
    )(x_out, keys, values)


def solution(mesh):
    n_tp, n_cp = mesh.shape['tp'], mesh.shape['cp']
    row_spec = P(('dp', 'cp'), None)
    cache_spec = P(('dp', 'cp'), 'tp', None)
    col_spec = P(None, 'tp')
    split_rows = P('tp', None)
    vec_spec = P(None)

    def local_layer(x, attn_gain, w_q, w_k, w_v, w_o, mlp_gain, w_gate, w_up, w_down):
        keys, values, hidden, normed = fused_attention(x, attn_gain, mlp_gain, w_q, w_k, w_v, w_o, n_tp, n_cp)
        x_out = fused_mlp(normed, hidden, w_gate, w_up, w_down, n_tp)
        return hand_over(x_out, keys, values)

    return jax.shard_map(local_layer, mesh=mesh,
                         in_specs=(row_spec, vec_spec, col_spec, col_spec, col_spec, split_rows, vec_spec, col_spec, col_spec, split_rows),
                         out_specs=(row_spec, cache_spec, cache_spec), check_vma=False)
```

```python
import functools
import math
import numpy as np
import jax
import jax.numpy as jnp
from jax import lax
from jax.experimental import pallas as pl
from jax.experimental.pallas import tpu as pltpu
from jax.sharding import PartitionSpec as P

HEAD_DIM = 128
OWN, LEFT, RIGHT, FAR = SLOTS = range(4)
LO, HI = BOTH = range(2)
KEY, VALUE = BOTH
KV_A, KV_B = BOTH
ROPE_THETA = 1000000.0
NORM_EPS = 1e-5
MASK_VALUE = -1e30
VMEM_LIMIT = 66000000
HALVES = 2
GROUPS_OUT = 4
COPY_BLOCKS = 8
FF_TILE = 256
OUT_TILE = 256
DN_BUFS = 3
PROJ_TILE = 256
Q_CHUNKS = 4
KX = 8
OUT_COLS = 2560
NORM_ROWS = 16
ANGLE_ROWS = 32


def attn_kernel(n_tp, n_cp, x_hbm, gain_ref, mlp_gain_ref, freq_ref, wq_hbm, wk_hbm, wv_hbm, wo_hbm,
                k_out, v_out, h_out, n_out,
                nbuf, wt, kbuf, vbuf, qt, part, relay, fin, hrow, nrow, orow, s0, s1, acc, m_st, l_st, cos_s, sin_s, bias, vnat, cache,
                xsem, wsem, wosem, hsem, osem, kvo_sem, kx_send, kx_recv, sb_send, sb_recv, rs_send, rs_recv):
    tok, D = nbuf.shape
    kv_n, HT = kbuf.shape[3], kbuf.shape[4]
    QC = tok // Q_CHUNKS
    QL = qt.shape[3]
    groups = QL // QC
    R = QC // n_tp
    H = R // 2
    lo, hi = pl.ds(0, H), pl.ds(H, H)
    me = lax.axis_index('tp')
    right = lax.rem(me + 1, n_tp)
    left = lax.rem(me + n_tp - 1, n_tp)
    far = lax.rem(me + 2, n_tp)
    cp = lax.axis_index('cp')
    core = lax.rem(cp, 2)
    chip = cp // 2
    last_chip = n_cp // 2 - 1
    sib = cp + 1 - 2 * core
    x_right = lax.rem(cp + 2, n_cp)
    x_left = lax.rem(cp + n_cp - 2, n_cp)
    cexp = (HEAD_DIM ** -0.5) * math.log2(math.e)
    f32, bf16 = jnp.float32, jnp.bfloat16
    s_buf = (s0, s1)

    def remote(src, dst, ssem, rsem, to):
        return pltpu.make_async_remote_copy(src_ref=src, dst_ref=dst, send_sem=ssem, recv_sem=rsem,
                                            device_id=to, device_id_type=pl.DeviceIdType.MESH)

    quarters = (pl.ds(0, QC), pl.ds(QC, QC))

    def kx(k, b):
        buf = (kbuf, vbuf)[b]
        src, dst, half, to, keys = ((OWN, LEFT, LO, x_right, quarters[LO]), (OWN, LEFT, HI, x_right, None),
                                    (OWN, RIGHT, LO, x_left, quarters[LO]), (OWN, RIGHT, HI, x_left, None),
                                    (LEFT, FAR, LO, x_right, None), (RIGHT, FAR, HI, x_left, None),
                                    (OWN, LEFT, LO, x_right, quarters[HI]), (OWN, RIGHT, LO, x_left, quarters[HI]))[k]
        refs = [buf.at[slot, LO, half] for slot in (src, dst)]
        if keys is not None:
            refs = [ref.at[:, :, keys] if b == VALUE else ref.at[:, keys] for ref in refs]
        return remote(*refs, kx_send.at[k, b], kx_recv.at[k, b], {'cp': to})

    RIGHT_MORE, LEFT_MORE = KX - 2, KX - 1

    def sb(rel, half, b):
        buf = (kbuf, vbuf)[b]
        return remote(buf.at[rel, LO, half], buf.at[rel, HI, half], sb_send.at[rel, half, b], sb_recv.at[rel, half, b], {'cp': sib})

    def rs(i, k):
        p = lax.rem(i, 2)
        src, dst, to = ((part.at[p, far, lo], relay.at[i, LO], right),
                        (part.at[p, far, hi], relay.at[i, HI], left),
                        (part.at[p, right, hi], fin.at[i, LO, hi], right),
                        (part.at[p, left, lo], fin.at[i, HI, lo], left),
                        (part.at[p, right, lo], fin.at[i, LO, lo], right),
                        (part.at[p, left, hi], fin.at[i, HI, hi], left))[k]
        return remote(src, dst, rs_send.at[i, k], rs_recv.at[i, k], {'tp': to})

    def x_load(c):
        rows = pl.ds(pl.multiple_of(c * QC, QC), QC)
        return pltpu.make_async_copy(x_hbm.at[rows], nbuf.at[rows], xsem.at[c])

    def w_load(ref, t, slot):
        return pltpu.make_async_copy(ref.at[:, pl.ds(pl.multiple_of(t * PROJ_TILE, PROJ_TILE), PROJ_TILE)], wt.at[slot], wsem.at[slot])

    def h_load(i):
        return pltpu.make_async_copy(x_hbm.at[pl.ds(pl.multiple_of(i * QC + me * R, R), R)], hrow.at[i], hsem.at[i])

    def o_store(i):
        rows = pl.ds(i * R, R)
        return (pltpu.make_async_copy(hrow.at[i], h_out.at[rows], osem.at[0, i]),
                pltpu.make_async_copy(nrow.at[i], n_out.at[rows], osem.at[1, i]))

    wo_load = pltpu.make_async_copy(wo_hbm, nbuf, wosem)

    x_load(0).start()
    barrier = pltpu.get_barrier_semaphore()
    for to in ({'tp': left}, {'tp': right}, {'cp': x_left}, {'cp': x_right}, {'cp': sib}):
        pl.semaphore_signal(barrier, inc=1, device_id=to, device_id_type=pl.DeviceIdType.MESH)

    def make_tables():
        freq = freq_ref[...]

        def angles(step, base):
            t = lax.broadcasted_iota(jnp.int32, (ANGLE_ROWS, HEAD_DIM), 0) * step + base
            a = t.astype(f32) * freq
            return jnp.cos(a), jnp.sin(a)

        sign = jnp.where(lax.broadcasted_iota(jnp.int32, (1, HEAD_DIM), 1) < HEAD_DIM // 2, -1.0, 1.0)
        fine_cos, fine_sin = angles(1, 0)
        base_cos, base_sin = angles(ANGLE_ROWS, cp * tok)
        for b in range(tok // ANGLE_ROWS):
            ca, sa = base_cos[b:b + 1], base_sin[b:b + 1]
            rows = slice(b * ANGLE_ROWS, (b + 1) * ANGLE_ROWS)
            cos_s[rows, :] = ca * fine_cos - sa * fine_sin
            sin_s[rows, :] = (sa * fine_cos + ca * fine_sin) * sign

    def make_bias():
        key_at = lax.broadcasted_iota(jnp.int32, bias.shape[1:], 0)
        row_at = lax.broadcasted_iota(jnp.int32, bias.shape[1:], 1)
        for odd in BOTH:
            bias[odd] = jnp.where(key_at <= row_at + odd * QC, 0.0, MASK_VALUE)

    def normalize(wide, gain):
        inv = lax.rsqrt(jnp.mean(wide * wide, axis=-1, keepdims=True) + NORM_EPS)
        return (wide * inv * gain).astype(bf16)

    gain = gain_ref[...].astype(f32)[None, :]

    def stage(c):
        return nrow if c % 2 == 0 else part.at[0]

    def inv_rows(c, b):
        first = (c % 2) * QC + b * NORM_ROWS
        return slice(first, first + NORM_ROWS)

    def stat_chunk(c):
        for b in range(QC // NORM_ROWS):
            rows = slice(c * QC + b * NORM_ROWS, c * QC + (b + 1) * NORM_ROWS)
            wide = nbuf[rows, :].astype(f32)
            s0[inv_rows(c, b), 0:1] = lax.rsqrt(jnp.mean(wide * wide, axis=-1, keepdims=True) + NORM_EPS)

    def norm_chunk(c):
        for b in range(QC // NORM_ROWS):
            rows = slice(c * QC + b * NORM_ROWS, c * QC + (b + 1) * NORM_ROWS)
            scaled = (nbuf[rows, :].astype(f32) * s0[inv_rows(c, b), 0:1] * gain).astype(bf16)
            nbuf[rows, :] = scaled
            stage(c)[b * NORM_ROWS // R, b * NORM_ROWS % R:b * NORM_ROWS % R + NORM_ROWS, :] = scaled

    def rope(u, rows, scale=None):
        wide = u.astype(bf16).astype(f32)
        turned = wide * cos_s[rows, :] + pltpu.roll(wide, HEAD_DIM // 2, 1) * sin_s[rows, :]
        return (turned if scale is None else turned * scale).astype(bf16)

    x_load(0).wait()
    w_load(wk_hbm, 0, 0).start()
    w_load(wv_hbm, 0, 1).start()
    x_load(1).start()
    stat_chunk(0)
    norm_chunk(0)
    x_load(1).wait()
    x_load(2).start()
    x_load(3).start()
    stat_chunk(1)
    w_load(wk_hbm, 0, 0).wait()
    w_load(wv_hbm, 0, 1).wait()
    w_load(wq_hbm, 0, 2).start()
    for i in range(Q_CHUNKS):
        h_load(i).start()
    for c in range(Q_CHUNKS):
        rows = slice(c * QC, (c + 1) * QC)
        half = c // 2
        part_rows = slice((c % 2) * QC, (c % 2 + 1) * QC)
        if c + 2 < Q_CHUNKS:
            x_load(c + 2).wait()
        n_rows = stage(c)[...].reshape(QC, D)
        k_res = jnp.dot(n_rows, wt[0], preferred_element_type=f32)
        v_res = jnp.dot(n_rows, wt[1], preferred_element_type=f32).astype(bf16)
        if c == 0:
            make_tables()
        if c == Q_CHUNKS - 1:
            make_bias()
        if c + 1 < Q_CHUNKS:
            norm_chunk(c + 1)
        if c + 2 < Q_CHUNKS:
            stat_chunk(c + 2)
        vnat[rows, :] = v_res
        for j in range(kv_n):
            cols = slice(j * HEAD_DIM, (j + 1) * HEAD_DIM)
            head = rope(k_res[:, cols], rows)
            kbuf[OWN, LO, half, j, part_rows, :] = head
            vbuf[OWN, LO, half, j, :, part_rows] = v_res[:, cols].T
        if c == 0:
            pl.semaphore_wait(barrier, 5)
            for b in BOTH:
                kx(OWN, b).start()
                kx(2, b).start()
        if c == 1:
            for b in BOTH:
                kx(RIGHT_MORE, b).start()
                kx(LEFT_MORE, b).start()
                sb(OWN, LO, b).start()
    w_load(wq_hbm, 1, 0).start()
    w_load(wq_hbm, 2, 1).start()
    for b in BOTH:
        kx(1, b).start()
        kx(3, b).start()
        sb(OWN, HI, b).start()

    n_q = wq_hbm.shape[1] // PROJ_TILE
    heads_tile = PROJ_TILE // HEAD_DIM
    tiles_kv = n_q // kv_n

    def q_step(t, carry):
        slot = lax.rem(t + 2, 3)
        w_load(wq_hbm, t, slot).wait()
        res = jnp.dot(nbuf[...], wt[slot], preferred_element_type=f32)
        kv, base = t // tiles_kv, lax.rem(t, tiles_kv) * heads_tile
        for j in range(heads_tile):
            head = rope(res[:, j * HEAD_DIM:(j + 1) * HEAD_DIM], slice(None), cexp)
            lanes = pl.ds(pl.multiple_of((base + j) * QC, QC), QC)
            for i in range(Q_CHUNKS):
                qt[i, kv, :, lanes] = head[i * QC:(i + 1) * QC].T

        @pl.when(t + 3 < n_q)
        def _():
            w_load(wq_hbm, t + 3, slot).start()
        return carry
    lax.fori_loop(0, n_q, q_step, 0)
    wo_load.start()
    for b in BOTH:
        kx(OWN, b).wait_recv()
        kx(RIGHT_MORE, b).wait_recv()
        kx(4, b).start()
        sb(LEFT, LO, b).start()
        kx(2, b).wait_recv()
        kx(LEFT_MORE, b).wait_recv()
        sb(RIGHT, LO, b).start()
    for half in BOTH:
        for b in BOTH:
            sb(OWN, half, b).wait_recv()

    def ev_near():
        for b in BOTH:
            kx(1, b).wait_recv()
            sb(LEFT, HI, b).start()
            kx(3, b).wait_recv()
            kx(5, b).start()
            sb(RIGHT, HI, b).start()

    def ev_far():
        for b in BOTH:
            kx(4, b).wait_recv()
            sb(FAR, LO, b).start()
            kx(5, b).wait_recv()
            sb(FAR, HI, b).start()

    def ev_sib(rel):
        for half in BOTH:
            for b in BOTH:
                sb(rel, half, b).wait_recv()

    n_far = core + jnp.where(chip >= 1, 2, 0) + jnp.where(chip == last_chip, 2, 0)
    events = ((ev_near, core), (functools.partial(ev_sib, LEFT), core + 1),
              (functools.partial(ev_sib, RIGHT), jnp.where(chip == last_chip, core + 3, n_cp)),
              (ev_far, n_far), (functools.partial(ev_sib, FAR), n_far + 1))

    def block_of(n):
        own = n >= cp
        sib_block = (core == 1) & (n == 0)
        p = n - core
        pair = p // 2
        rel = jnp.where(own | sib_block, OWN, jnp.where(pair == OWN, LEFT, jnp.where(chip == last_chip, pair + 1, FAR)))
        which = jnp.where(own, LO, jnp.where(sib_block, HI, lax.rem(p + 2, 2)))
        return rel, which

    def scores(i, kv, tile, half):
        rel, which = tile
        s_buf[kv][...] = jnp.dot(kbuf[rel, which, half, kv], qt[i, kv], preferred_element_type=f32)

    def soft(kv, tile, half, off=None):
        first = off is not None
        rel, which = tile
        s = s_buf[kv][...]
        if first:
            s = s + jnp.concatenate([bias[off]] * groups, axis=1)
        m_new = jnp.max(s, axis=0, keepdims=True)
        if not first:
            m_old = m_st[kv]
            m_new = jnp.maximum(m_old, m_new)
            alpha = jnp.exp2(m_old - m_new)
        p = jnp.exp2(s - m_new)
        total = jnp.sum(p, axis=0, keepdims=True)
        add = jnp.dot(vbuf[rel, which, half, kv], p.astype(bf16), preferred_element_type=f32)
        m_st[kv] = m_new
        if first:
            l_st[kv] = total
            acc[kv] = add
        else:
            l_st[kv] = l_st[kv] * alpha + total
            acc[kv] = acc[kv] * alpha + add

    def m0(i):
        for k in range(4):
            rs(i, k).start()

    def m1(i):
        p = lax.rem(i, 2)
        for j, owner, rows in ((LO, right, lo), (HI, left, hi)):
            rs(i, j).wait_recv()
            part[p, owner, rows, :] = (part[p, owner, rows, :].astype(f32) + relay[i, j].astype(f32)).astype(bf16)
        rs(i, 4).start()
        rs(i, 5).start()

    mlp_gain = mlp_gain_ref[...].astype(f32)[None, :]

    def m2(i):
        p = lax.rem(i, 2)
        for k in range(2, 6):
            rs(i, k).wait_recv()
        for k in range(6):
            rs(i, k).wait_send()
        total = part[p, me].astype(f32) + fin[i, LO].astype(f32) + fin[i, HI].astype(f32)
        hid = (hrow[i].astype(f32) + total).astype(bf16)
        hrow[i] = hid
        nrow[i] = normalize(hid.astype(f32), mlp_gain)
        for c in o_store(i):
            c.start()

    def chunk(i, carry):
        first, later, before = i == 0, i > 0, i - 1
        def waits_at(block):
            return first & functools.reduce(jnp.logical_or, [block == at for _, at in events])

        def ahead(block):
            stop = waits_at(block)
            rel, which = block_of(block)
            return jnp.where(stop, OWN, rel), jnp.where(stop, LO, which)
        own = (OWN, LO)
        first_block = ahead(0)
        off = lax.rem(i, 2)
        late = i // 2

        def diag_step(_, c2):
            scores(i, KV_A, own, late)
            scores(i, KV_B, own, late)
            soft(KV_A, own, late, off)
            scores(i, KV_A, (jnp.where(late == 1, 0, first_block[0]), jnp.where(late == 1, 0, first_block[1])), 0)
            soft(KV_B, own, late, off)
            return c2
        lax.fori_loop(0, 1, diag_step, 0)

        def own_step(_, c2):
            scores(i, KV_B, own, LO)
            soft(KV_A, own, LO)
            scores(i, KV_A, first_block, LO)
            soft(KV_B, own, LO)
            return c2
        lax.fori_loop(0, late, own_step, 0)

        def pair_step(n, c2):
            @pl.when(waits_at(n))
            def _():
                for fn, at in events:
                    pl.when(n == at)(fn)
                scores(i, KV_A, block_of(n), LO)

            @pl.when(later & (n == cp // 2))
            def _():
                m1(before)
            blk = block_of(n)
            scores(i, KV_B, blk, LO)
            soft(KV_A, blk, LO)
            scores(i, KV_A, blk, HI)
            soft(KV_B, blk, LO)
            scores(i, KV_B, blk, HI)
            soft(KV_A, blk, HI)
            scores(i, KV_A, ahead(n + 1), LO)
            soft(KV_B, blk, HI)
            return c2
        lax.fori_loop(0, cp, pair_step, 0)

        @pl.when(first)
        def _():
            for fn, at in events:
                pl.when(at >= cp)(fn)
            wo_load.wait()

        @pl.when(later & (cp == 0))
        def _():
            m1(before)
        for kv in range(kv_n):
            inv = 1.0 / l_st[kv]
            for g in range(groups):
                lanes = slice(g * QC, (g + 1) * QC)
                h = kv * groups + g
                orow[:, h * HEAD_DIM:(h + 1) * HEAD_DIM] = (acc[kv, :, lanes] * inv[:, lanes]).astype(bf16).T
        p = lax.rem(i, 2)

        def out_step(j, c2):
            cols = pl.ds(pl.multiple_of(j * OUT_COLS, OUT_COLS), OUT_COLS)
            part[p, :, :, cols] = jnp.dot(orow[...], nbuf[:, cols], preferred_element_type=f32).astype(bf16).reshape(n_tp, R, OUT_COLS)
            return c2
        lax.fori_loop(0, D // OUT_COLS, out_step, 0)
        m0(i)

        @pl.when(later)
        def _():
            h_load(before).wait()
            m2(before)
        return carry
    lax.fori_loop(0, Q_CHUNKS, chunk, 0)
    last = Q_CHUNKS - 1
    for n, out in enumerate((k_out, v_out)):
        for j in range(kv_n):
            if n:
                cache[:, j, :] = vnat[:, j * HEAD_DIM:(j + 1) * HEAD_DIM]
            else:
                for half in BOTH:
                    cache[half * HT:(half + 1) * HT, j, :] = kbuf[OWN, LO, half, j]
        stored = pltpu.make_async_copy(cache, out, kvo_sem.at[n])
        stored.start()
        stored.wait()
    m1(last)
    h_load(last).wait()
    m2(last)
    for b in BOTH:
        for k in range(KX):
            kx(k, b).wait_send()
        for rel in range(n_cp // 2):
            for half in BOTH:
                sb(rel, half, b).wait_send()
    for i in range(Q_CHUNKS):
        for c in o_store(i):
            c.wait()


def fused_attention(x, attn_gain, mlp_gain, w_q, w_k, w_v, w_o, n_tp, n_cp):
    tok, D = x.shape
    kv_n = w_k.shape[1] // HEAD_DIM
    groups = w_q.shape[1] // w_k.shape[1]
    QC = tok // Q_CHUNKS
    QL = QC * groups
    R = QC // n_tp
    H = R // 2
    HT = tok // 2
    bf, f32 = jnp.bfloat16, jnp.float32
    anys = pl.BlockSpec(memory_space=pl.ANY)
    vm = pl.BlockSpec(memory_space=pltpu.VMEM)
    own = tok // n_tp
    dma = pltpu.SemaphoreType.DMA
    inv_freq = ROPE_THETA ** (-np.arange(0, HEAD_DIM, 2) / HEAD_DIM)
    freq = jnp.asarray(np.concatenate([inv_freq, inv_freq])[None, :], f32)
    return pl.pallas_call(
        functools.partial(attn_kernel, n_tp, n_cp),
        out_shape=(jax.ShapeDtypeStruct((tok, kv_n, HEAD_DIM), bf), jax.ShapeDtypeStruct((tok, kv_n, HEAD_DIM), bf),
                   jax.ShapeDtypeStruct((own, D), bf), jax.ShapeDtypeStruct((own, D), bf)),
        in_specs=[anys, vm, vm, vm, anys, anys, anys, anys],
        out_specs=(anys,) * 4,
        scratch_shapes=[
            pltpu.VMEM((tok, D), bf),
            pltpu.VMEM((3, D, PROJ_TILE), bf),
            pltpu.VMEM((n_cp // 2, 2, 2, kv_n, HT, HEAD_DIM), bf),
            pltpu.VMEM((n_cp // 2, 2, 2, kv_n, HEAD_DIM, HT), bf),
            pltpu.VMEM((Q_CHUNKS, kv_n, HEAD_DIM, QL), bf),
            pltpu.VMEM((2, n_tp, R, D), bf),
            pltpu.VMEM((Q_CHUNKS, 2, H, D), bf),
            pltpu.VMEM((Q_CHUNKS, 2, R, D), bf),
            pltpu.VMEM((Q_CHUNKS, R, D), bf),
            pltpu.VMEM((Q_CHUNKS, R, D), bf),
            pltpu.VMEM((QC, kv_n * groups * HEAD_DIM), bf),
            pltpu.VMEM((HT, QL), f32),
            pltpu.VMEM((HT, QL), f32),
            pltpu.VMEM((kv_n, HEAD_DIM, QL), f32),
            pltpu.VMEM((kv_n, 1, QL), f32),
            pltpu.VMEM((kv_n, 1, QL), f32),
            pltpu.VMEM((tok, HEAD_DIM), f32),
            pltpu.VMEM((tok, HEAD_DIM), f32),
            pltpu.VMEM((2, HT, QC), f32),
            pltpu.VMEM((tok, kv_n * HEAD_DIM), bf),
            pltpu.VMEM((tok, kv_n, HEAD_DIM), bf),
            dma((Q_CHUNKS,)), dma((3,)), dma, dma((Q_CHUNKS,)), dma((2, Q_CHUNKS)), dma((2,)),
            dma((KX, 2)), dma((KX, 2)), dma((n_cp // 2, 2, 2)), dma((n_cp // 2, 2, 2)), dma((Q_CHUNKS, 6)), dma((Q_CHUNKS, 6)),
        ],
        compiler_params=pltpu.CompilerParams(collective_id=1, has_side_effects=True, vmem_limit_bytes=VMEM_LIMIT),
        name='fused_attention',
    )(x, attn_gain, mlp_gain, freq, w_q, w_k, w_v, w_o)


def mlp_kernel(n_tp, n_hbm, h_hbm, wg_hbm, wu_hbm, wd_hbm, out_hbm,
               nbuf, act, wg_buf, wu_buf, wd_buf, part, relay, fin, xfin, h_ref,
               h_sem, wsem, dsem, own_sem, ag_send, ag_recv, rs_send, rs_recv, go_send, go_recv, loc_sem):
    me = lax.axis_index('tp')
    right = lax.rem(me + 1, n_tp)
    left = lax.rem(me + n_tp - 1, n_tp)
    _, _, R, D = nbuf.shape
    H = R // 2
    DG = part.shape[-1]
    n_ff = act.shape[1] // FF_TILE
    n_out = D // OUT_TILE
    per_group = DG // OUT_TILE
    lo, hi = pl.ds(0, H), pl.ds(H, H)

    def remote(src, dst, ssem, rsem, to):
        return pltpu.make_async_remote_copy(src_ref=src, dst_ref=dst, send_sem=ssem, recv_sem=rsem,
                                            device_id={'tp': to}, device_id_type=pl.DeviceIdType.MESH)

    def ag(s, k):
        src_slot, dst_slot, rows, to = ((OWN, LEFT, lo, right), (OWN, LEFT, hi, right), (OWN, RIGHT, hi, left), (OWN, RIGHT, lo, left),
                                        (LEFT, FAR, lo, right), (RIGHT, FAR, hi, left))[k]
        return remote(nbuf.at[s, src_slot, rows], nbuf.at[s, dst_slot, rows], ag_send.at[s, k], ag_recv.at[s, k], to)

    def rs(s, g, k):
        src, dst, to = ((part.at[s, g, FAR, lo], relay.at[s, g, LO], right),
                        (part.at[s, g, FAR, hi], relay.at[s, g, HI], left),
                        (part.at[s, g, RIGHT, hi], fin.at[s, g, LO, hi], right),
                        (part.at[s, g, LEFT, lo], fin.at[s, g, HI, lo], left),
                        (part.at[s, g, RIGHT, lo], fin.at[s, g, LO, lo], right),
                        (part.at[s, g, LEFT, hi], fin.at[s, g, HI, hi], left))[k]
        return remote(src, dst, rs_send.at[s, g, k], rs_recv.at[s, g, k], to)

    def out_rows(owner, s, half):
        return pl.ds(pl.multiple_of(((HALVES * s + half) * n_tp + owner) * H, H), H)

    def go(s, g, k):
        cols = pl.ds(g * DG, DG)
        half = (LO, HI, HI, LO, LO, HI)[k]
        to = (right, right, left, left, right, left)[k]
        owner = (me, me, me, me, left, right)[k]
        dst = out_hbm.at[out_rows(owner, s, half), cols]
        src = xfin.at[s, g, pl.ds(half * H, H)] if k < 4 else dst
        return remote(src, dst, go_send.at[s, g, k], go_recv.at[s, g, k], to)

    def loc(s, g, half):
        return pltpu.make_async_copy(xfin.at[s, g, pl.ds(half * H, H)], out_hbm.at[out_rows(me, s, half), pl.ds(g * DG, DG)],
                                     loc_sem.at[s, g, half])

    def own(s):
        return pltpu.make_async_copy(n_hbm.at[pl.ds(s * R, R)], nbuf.at[s, 0], own_sem.at[s])

    def gu_load(t, slot):
        cols = pl.ds(pl.multiple_of(t * FF_TILE, FF_TILE), FF_TILE)
        return (pltpu.make_async_copy(wg_hbm.at[:, cols], wg_buf.at[slot], wsem.at[0, slot]),
                pltpu.make_async_copy(wu_hbm.at[:, cols], wu_buf.at[slot], wsem.at[1, slot]))

    def dn_load(j, slot):
        cols = pl.ds(pl.multiple_of(j * OUT_TILE, OUT_TILE), OUT_TILE)
        return pltpu.make_async_copy(wd_hbm.at[:, cols], wd_buf.at[slot], dsem.at[slot])

    def gu_first():
        for t in range(2):
            for c in gu_load(t, t):
                c.start()

    def dn_first():
        for j in range(DN_BUFS):
            dn_load(j, j).start()

    for s in range(HALVES):
        own(s).start()
    gu_first()
    barrier = pltpu.get_barrier_semaphore()
    for nbr in (left, right):
        pl.semaphore_signal(barrier, inc=1, device_id={'tp': nbr}, device_id_type=pl.DeviceIdType.MESH)
    pl.semaphore_wait(barrier, 2)

    def ag_own(s):
        own(s).wait()
        for k in range(4):
            ag(s, k).start()

    def ag_fwd(s, k):
        ag(s, k).wait_recv()
        ag(s, 4 + k // 2).start()

    def ag_rest(s):
        for k in (1, 3, 4, 5):
            ag(s, k).wait_recv()

    def m0(s, g):
        for k in range(4):
            rs(s, g, k).start()

    def m1(s, g):
        for i, slot, rows in ((LO, RIGHT, lo), (HI, LEFT, hi)):
            rs(s, g, i).wait_recv()
            total = part[s, g, slot, rows, :].astype(jnp.float32) + relay[s, g, i].astype(jnp.float32)
            part[s, g, slot, rows, :] = total.astype(jnp.bfloat16)
        rs(s, g, 4).start()
        rs(s, g, 5).start()

    def m2(s, g):
        for k in range(2, 6):
            rs(s, g, k).wait_recv()
        total = (part[s, g, OWN].astype(jnp.float32) + fin[s, g, LO].astype(jnp.float32)) + fin[s, g, HI].astype(jnp.float32)
        res = h_ref[pl.ds(s * R, R), pl.ds(g * DG, DG)].astype(jnp.float32)
        xfin[s, g] = (res + total).astype(jnp.bfloat16)
        for k in range(4):
            go(s, g, k).start()
        for half in BOTH:
            loc(s, g, half).start()

    def m3(s, g):
        go(s, g, 0).wait_recv()
        go(s, g, 4).start()
        go(s, g, 2).wait_recv()
        go(s, g, 5).start()

    def gate_up(s, first, count, hooks):
        def step(t, carry):
            slot = lax.rem(t, 2)
            for c in gu_load(t, slot):
                c.wait()
            rows = nbuf[s, first:first + count].reshape(count * R, D)
            gate = jnp.dot(rows, wg_buf[slot], preferred_element_type=jnp.float32)
            up = jnp.dot(rows, wu_buf[slot], preferred_element_type=jnp.float32)
            act[first * R:(first + count) * R, pl.ds(pl.multiple_of(t * FF_TILE, FF_TILE), FF_TILE)] = (jax.nn.silu(gate) * up).astype(jnp.bfloat16)

            @pl.when(t + 2 < n_ff)
            def _():
                for c in gu_load(t + 2, slot):
                    c.start()
            for at, fn in hooks:
                pl.when(t == at)(fn)
            return carry
        lax.fori_loop(0, n_ff, step, 0)

    def down(s, hooks):
        def step(j, carry):
            slot = lax.rem(j, DN_BUFS)
            dn_load(j, slot).wait()
            res = jnp.dot(act[...], wd_buf[slot], preferred_element_type=jnp.float32).astype(jnp.bfloat16)
            g, c = j // per_group, lax.rem(j, per_group)
            part[s, g, :, :, pl.ds(pl.multiple_of(c * OUT_TILE, OUT_TILE), OUT_TILE)] = res.reshape(4, R, OUT_TILE)

            @pl.when(j + DN_BUFS < n_out)
            def _():
                dn_load(j + DN_BUFS, slot).start()
            for at, fn in hooks:
                pl.when(j == at)(fn)
            return carry
        lax.fori_loop(0, n_out, step, 0)

    P_ = functools.partial
    G = GROUPS_OUT
    ag_own(0)

    def feed():
        ag_fwd(0, 0)
        ag_fwd(0, 2)
        ag_own(1)
    dn_first()
    h_load = pltpu.make_async_copy(h_hbm, h_ref, h_sem)
    h_load.start()
    gate_up(0, 0, 1, [(7, feed)])
    h_load.wait()
    gu_first()
    ag_rest(0)
    gate_up(0, 1, 3, [(7, P_(ag_fwd, 1, 0)), (8, P_(ag_fwd, 1, 2))])
    gu_first()
    send_hooks = lambda s: [(per_group * (g + 1), P_(m0, s, g)) for g in range(G - 1)]
    down(0, send_hooks(0) + [(13, P_(m1, 0, 0)), (18, P_(m1, 0, 1))])
    m0(0, G - 1)
    dn_first()
    ag_rest(1)
    gate_up(1, 0, 4, [(1, P_(m1, 0, 2)), (4, P_(m1, 0, 3))] + [(6 + 2 * g, P_(m2, 0, g)) for g in range(G)])
    down(1, send_hooks(1) + [(per_group * g + 2, P_(m3, 0, g)) for g in range(G)] + [(13, P_(m1, 1, 0)), (18, P_(m1, 1, 1))])
    m0(1, G - 1)
    m1(1, 2)
    m1(1, 3)
    m2(1, 0)
    m2(1, 1)
    m3(1, 0)
    m2(1, 2)
    m3(1, 1)
    m2(1, 3)
    m3(1, 2)
    m3(1, 3)
    for s in range(HALVES):
        for k in range(6):
            ag(s, k).wait_send()
        for g in range(G):
            for half in BOTH:
                loc(s, g, half).wait()
            for k in range(6):
                rs(s, g, k).wait_send()
                go(s, g, k).wait_send()
            for k in (1, 3, 4, 5):
                go(s, g, k).wait_recv()


def fused_mlp(normed, hidden, w_gate, w_up, w_down, n_tp):
    own_rows, D = normed.shape
    F = w_gate.shape[1]
    R = own_rows // HALVES
    H = R // 2
    DG = D // GROUPS_OUT
    bf = jnp.bfloat16
    S, G = HALVES, GROUPS_OUT
    anys = pl.BlockSpec(memory_space=pl.ANY)
    return pl.pallas_call(
        functools.partial(mlp_kernel, n_tp),
        out_shape=jax.ShapeDtypeStruct((own_rows * n_tp, D), bf),
        in_specs=[anys] * 5,
        out_specs=anys,
        scratch_shapes=[
            pltpu.VMEM((S, 4, R, D), bf),
            pltpu.VMEM((4 * R, F), bf),
            pltpu.VMEM((2, D, FF_TILE), bf),
            pltpu.VMEM((2, D, FF_TILE), bf),
            pltpu.VMEM((DN_BUFS, F, OUT_TILE), bf),
            pltpu.VMEM((S, G, 4, R, DG), bf),
            pltpu.VMEM((S, G, 2, H, DG), bf),
            pltpu.VMEM((S, G, 2, R, DG), bf),
            pltpu.VMEM((S, G, R, DG), bf),
            pltpu.VMEM((own_rows, D), bf),
            pltpu.SemaphoreType.DMA,
            pltpu.SemaphoreType.DMA((2, 2)),
            pltpu.SemaphoreType.DMA((DN_BUFS,)),
            pltpu.SemaphoreType.DMA((S,)),
            pltpu.SemaphoreType.DMA((S, 6)),
            pltpu.SemaphoreType.DMA((S, 6)),
            pltpu.SemaphoreType.DMA((S, G, 6)),
            pltpu.SemaphoreType.DMA((S, G, 6)),
            pltpu.SemaphoreType.DMA((S, G, 6)),
            pltpu.SemaphoreType.DMA((S, G, 6)),
            pltpu.SemaphoreType.DMA((S, G, 2)),
        ],
        compiler_params=pltpu.CompilerParams(collective_id=0, has_side_effects=True, vmem_limit_bytes=VMEM_LIMIT),
        cost_estimate=pl.CostEstimate(flops=2 * own_rows * n_tp * D * F * 3, bytes_accessed=2 * 3 * 2 * D * F, transcendentals=0),
        name='fused_mlp',
    )(normed, hidden, w_gate, w_up, w_down)


def hand_over_kernel(x_in, k_in, v_in, x_out, k_out, v_out, x_buf, k_buf, v_buf, in_sem, out_sem):
    n_blocks, rows, _ = x_buf.shape
    copies = []
    for b in range(n_blocks):
        at = pl.ds(b * rows, rows)
        copies.append((pltpu.make_async_copy(x_in.at[at], x_buf.at[b], in_sem.at[b]), pltpu.make_async_copy(x_buf.at[b], x_out.at[at], out_sem.at[b])))
    for n, (src, buf, dst) in enumerate(((k_in, k_buf, k_out), (v_in, v_buf, v_out))):
        copies.append((pltpu.make_async_copy(src, buf, in_sem.at[n_blocks + n]), pltpu.make_async_copy(buf, dst, out_sem.at[n_blocks + n])))
    for load, _ in copies:
        load.start()
    for load, store in copies:
        load.wait()
        store.start()
    for _, store in copies:
        store.wait()


def hand_over(x_out, keys, values):
    rows, D = x_out.shape
    bf = jnp.bfloat16
    block = rows // COPY_BLOCKS
    anys = pl.BlockSpec(memory_space=pl.ANY)
    dma = pltpu.SemaphoreType.DMA((COPY_BLOCKS + 2,))
    return pl.pallas_call(
        hand_over_kernel,
        out_shape=tuple(jax.ShapeDtypeStruct(a.shape, bf) for a in (x_out, keys, values)),
        in_specs=[anys] * 3,
        out_specs=(anys,) * 3,
        scratch_shapes=[pltpu.VMEM((COPY_BLOCKS, block, D), bf), pltpu.VMEM(keys.shape, bf), pltpu.VMEM(values.shape, bf), dma, dma],
        compiler_params=pltpu.CompilerParams(vmem_limit_bytes=VMEM_LIMIT),
        name='hand_over',
    )(x_out, keys, values)


def solution(mesh):
    n_tp, n_cp = mesh.shape['tp'], mesh.shape['cp']
    row_spec = P(('dp', 'cp'), None)
    cache_spec = P(('dp', 'cp'), 'tp', None)
    col_spec = P(None, 'tp')
    split_rows = P('tp', None)
    vec_spec = P(None)

    def local_layer(x, attn_gain, w_q, w_k, w_v, w_o, mlp_gain, w_gate, w_up, w_down):
        keys, values, hidden, normed = fused_attention(x, attn_gain, mlp_gain, w_q, w_k, w_v, w_o, n_tp, n_cp)
        x_out = fused_mlp(normed, hidden, w_gate, w_up, w_down, n_tp)
        return hand_over(x_out, keys, values)

    return jax.shard_map(local_layer, mesh=mesh,
                         in_specs=(row_spec, vec_spec, col_spec, col_spec, col_spec, split_rows, vec_spec, col_spec, col_spec, split_rows),
                         out_specs=(row_spec, cache_spec, cache_spec), check_vma=False)
```
